64 devices in a mesh: data: 4 (over x, y), ctx: 16 (over z, core).
Axes of the slice: x: 2, y: 2, z: 8, core: 2. Of those that a mesh axis runs over, the one named last changes fastest.
The devices are a block of a 4x4x8 slice.
Arguments:
- queries: bfloat16 [24, 6144, 8, 128], P('data', 'ctx'), parts along dimension 0
- keys_in: bfloat16 [24, 6144, 1, 128], P('data', 'ctx'), parts along dimension 0
- values_in: bfloat16 [24, 6144, 1, 128], P('data', 'ctx'), parts along dimension 0
- grad_out: bfloat16 [24, 6144, 8, 128], P('data', 'ctx'), parts along dimension 0
Outputs:
- output 1: bfloat16 [24, 6144, 8, 128], P('data', 'ctx'), parts along dimension 0
- output 2: bfloat16 [24, 6144, 8, 128], P('data', 'ctx'), parts along dimension 0
- output 3: bfloat16 [24, 6144, 1, 128], P('data', 'ctx'), parts along dimension 0
- output 4: bfloat16 [24, 6144, 1, 128], P('data', 'ctx'), parts along dimension 0
There are 4 independent parts. The reference program is written for one: setup_inputs(seed, part) draws one part's arguments, and reference() takes and returns one part's arrays. A program takes and returns all parts, laid end to end along the dimension named above; each array names one.
All inputs are finite; a program needn't handle non-finite values.
Results may differ from the reference program's by a relative error of at most 0.0171987.
Values are sent between devices in bfloat16 or wider.
A program may use at most 768 MiB of HBM per device.

```python
import jax
import jax.numpy as jnp
from jax import lax

BATCH = 6
TOKENS_DEV = 384
CTX_DEVICES = 16
Q_LOCAL = 8
KV_LOCAL = 1
HEAD_DIM = 128

SEQ_LEN = CTX_DEVICES * TOKENS_DEV
HALF_LEN = TOKENS_DEV // 2
NUM_PIECES = 2 * CTX_DEVICES
GROUP_SIZE = Q_LOCAL // KV_LOCAL
SPREAD = 1.6


def true_positions():
    token_index = jnp.arange(SEQ_LEN, dtype=jnp.int32)
    shard_id = token_index // TOKENS_DEV
    offset = token_index % TOKENS_DEV
    low_pos = shard_id * HALF_LEN + offset
    high_pos = (NUM_PIECES - 1 - shard_id) * HALF_LEN + offset - HALF_LEN
    return jnp.where(offset < HALF_LEN, low_pos, high_pos)


def setup_inputs(seed: int = 0, part: int = 0) -> dict:
    base_key = jax.random.fold_in(jax.random.key(seed), part)
    key_q, key_k, key_v, key_g = jax.random.split(base_key, 4)
    q_shape = (BATCH, SEQ_LEN, Q_LOCAL, HEAD_DIM)
    kv_shape = (BATCH, SEQ_LEN, KV_LOCAL, HEAD_DIM)
    queries = SPREAD * jax.random.normal(key_q, q_shape, jnp.float32)
    keys_in = SPREAD * jax.random.normal(key_k, kv_shape, jnp.float32)
    values_in = jax.random.normal(key_v, kv_shape, jnp.float32)
    grad_out = jax.random.normal(key_g, q_shape, jnp.float32)
    return {"queries": queries.astype(jnp.bfloat16), "keys_in": keys_in.astype(jnp.bfloat16), "values_in": values_in.astype(jnp.bfloat16), "grad_out": grad_out.astype(jnp.bfloat16)}


def reference(queries, keys_in, values_in, grad_out):
    score_scale = HEAD_DIM ** -0.5
    positions = true_positions()
    block_pos = positions.reshape(NUM_PIECES, HALF_LEN)
    keys_wide = keys_in.astype(jnp.float32)
    values_wide = values_in.astype(jnp.float32)

    def to_blocks(tensor):
        return tensor.reshape(BATCH, NUM_PIECES, HALF_LEN, KV_LOCAL, GROUP_SIZE, HEAD_DIM).transpose(1, 0, 2, 3, 4, 5)

    def from_blocks(tensor):
        return tensor.transpose(1, 0, 2, 3, 4, 5).reshape(BATCH, SEQ_LEN, Q_LOCAL, HEAD_DIM)

    def masked_scores(q_blk, pos_blk):
        raw_scores = jnp.einsum("bqhgd,bkhd->bhgqk", q_blk.astype(jnp.float32), keys_wide) * score_scale
        visible = pos_blk[:, None] >= positions[None, :]
        return jnp.where(visible, raw_scores, -jnp.inf)

    def forward_block(blk_args):
        q_blk, pos_blk = blk_args
        masked = masked_scores(q_blk, pos_blk)
        row_max = jnp.max(masked, axis=-1)
        row_sum = jnp.sum(jnp.exp(masked - row_max[..., None]), axis=-1)
        log_sum = row_max + jnp.log(row_sum)
        prob_tile = jnp.exp(masked - log_sum[..., None]).astype(jnp.bfloat16).astype(jnp.float32)
        out_blk = jnp.einsum("bhgqk,bkhd->bqhgd", prob_tile, values_wide)
        return out_blk.astype(jnp.bfloat16), log_sum

    q_blocks = to_blocks(queries)
    g_blocks = to_blocks(grad_out)
    out_blocks, lse_blocks = lax.map(forward_block, (q_blocks, block_pos))
    d_rows = jnp.einsum("nbqhgd,nbqhgd->nbhgq", g_blocks.astype(jnp.float32), out_blocks.astype(jnp.float32))

    def backward_step(loop_carry, blk_args):
        dk_acc, dv_acc = loop_carry
        q_blk, g_blk, lse_blk, drow_blk, pos_blk = blk_args
        q_wide = q_blk.astype(jnp.float32)
        g_wide = g_blk.astype(jnp.float32)
        prob_tile = jnp.exp(masked_scores(q_blk, pos_blk) - lse_blk[..., None])
        prob_low = prob_tile.astype(jnp.bfloat16).astype(jnp.float32)
        dv_acc = dv_acc + jnp.einsum("bhgqk,bqhgd->bkhd", prob_low, g_wide)
        dprob_tile = jnp.einsum("bqhgd,bkhd->bhgqk", g_wide, values_wide)
        dscore_tile = (prob_tile * (dprob_tile - drow_blk[..., None])).astype(jnp.bfloat16).astype(jnp.float32)
        dq_blk = jnp.einsum("bhgqk,bkhd->bqhgd", dscore_tile, keys_wide) * score_scale
        dk_acc = dk_acc + jnp.einsum("bhgqk,bqhgd->bkhd", dscore_tile, q_wide) * score_scale
        return (dk_acc, dv_acc), dq_blk.astype(jnp.bfloat16)

    zeros_kv = jnp.zeros((BATCH, SEQ_LEN, KV_LOCAL, HEAD_DIM), jnp.float32)
    grads_kv, dq_blocks = lax.scan(backward_step, (zeros_kv, zeros_kv), (q_blocks, g_blocks, lse_blocks, d_rows, block_pos))
    return (from_blocks(out_blocks), from_blocks(dq_blocks), grads_kv[0].astype(jnp.bfloat16), grads_kv[1].astype(jnp.bfloat16))
```

```python
import functools
import math

import jax
import jax.numpy as jnp
from jax import lax
from jax.experimental import pallas as pl
from jax.experimental.pallas import tpu as pltpu
from jax.sharding import PartitionSpec as P

MASK_VALUE = -1e30
BIG = 1024
SUB = 256
POS = 64
VMEM_BYTES = 60 * 2**20


def _dot(lhs, rhs):
    return lax.dot_general(lhs, rhs, (((1,), (0,)), ((), ())), preferred_element_type=jnp.float32)


def _attention_sequence(my_index, ctx_size, heads, q_ref, g_ref, k_ref, v_ref, o_ref, dq_ref, dk_ref, dv_ref, work):
    kt_ref, vt_ref, strip, qt_ref, gt_ref, ot_ref, dqt_ref, m_ref, l_ref = work
    seq_len, head_dim = k_ref.shape
    rows = q_ref.shape[0]
    half_len = rows // heads // 2
    tile = POS * heads
    scale = head_dim**-0.5
    log2_scale = scale * math.log2(math.e)
    last_piece = 2 * ctx_size - 1

    def prepare(step, carry):
        span = pl.ds(pl.multiple_of(step * BIG, BIG), BIG)
        kt_ref[:, span] = k_ref[span, :].T
        vt_ref[:, span] = v_ref[span, :].T
        dk_ref[span, :] = jnp.zeros((BIG, head_dim), jnp.float32)
        dv_ref[span, :] = jnp.zeros((BIG, head_dim), jnp.float32)
        return carry

    lax.fori_loop(0, seq_len // BIG, prepare, 0)

    def wide(row):
        return jnp.broadcast_to(row, (8, tile))

    def fold(block):
        return block.reshape(block.shape[0] // 8, 8, tile)

    def pair(pair_index, carry):
        low_subs = (my_index * half_len + POS * (pair_index + 1) - 1) // SUB + 1

        def geometry(half):
            piece = my_index + half * (last_piece - 2 * my_index)
            bound = piece * half_len + POS * (pair_index + 1)
            full_subs = (bound - 1) // SUB
            row = pl.multiple_of(half * (rows // 2) + pair_index * tile, tile)
            return bound, full_subs // (BIG // SUB), full_subs % (BIG // SUB), half * low_subs * SUB, row

        def score_block(half, key, at, size, row, bound):
            run_max = m_ref[half]
            for sub in range(0, size, SUB):
                scores = _dot(k_ref[pl.ds(key + sub, SUB), :], qt_ref[half])
                if bound is not None and sub + SUB == size:
                    key_pos = key + sub + lax.broadcasted_iota(jnp.int32, (SUB, 1), 0)
                    query_pos = bound - POS + lax.broadcasted_iota(jnp.int32, (1, tile), 1) // heads
                    scores = jnp.where(key_pos <= query_pos, scores, MASK_VALUE)
                strip[pl.ds(at + sub, SUB), :] = scores
                run_max = jnp.maximum(run_max, jnp.max(fold(scores), axis=0))
            m_ref[half] = run_max

        def value_block(half, key, at, size, row, bound):
            run_sum, shift, total = l_ref[half], m_ref[half], None
            for sub in range(0, size, SUB):
                probs = jnp.exp2(fold(strip[pl.ds(at + sub, SUB), :]) * log2_scale - shift[None])
                run_sum = run_sum + jnp.sum(probs, axis=0)
                part = _dot(vt_ref[:, pl.ds(key + sub, SUB)], probs.reshape(SUB, tile).astype(jnp.bfloat16))
                total = part if total is None else total + part
            l_ref[half] = run_sum
            ot_ref[half] += total

        def grad_block(half, key, at, size, row, bound):
            log_sum, d_row, total = m_ref[half], l_ref[half], None
            for sub in range(0, size, SUB):
                span = pl.ds(key + sub, SUB)
                dprobs = _dot(v_ref[span, :], gt_ref[half])
                probs = jnp.exp2(fold(strip[pl.ds(at + sub, SUB), :]) * log2_scale - log_sum[None])
                dscores = probs * (fold(dprobs) - d_row[None])
                probs = probs.reshape(SUB, tile).astype(jnp.bfloat16)
                dscores = dscores.reshape(SUB, tile).astype(jnp.bfloat16)
                dv_ref[span, :] += _dot(probs, g_ref[pl.ds(row, tile), :])
                dk_ref[span, :] += _dot(dscores, q_ref[pl.ds(row, tile), :])
                part = _dot(kt_ref[:, span], dscores)
                total = part if total is None else total + part
            dqt_ref[half] += total

        def sweep(half, block):
            bound, full_steps, rest_subs, start, row = geometry(half)

            def step(index, inner):
                block(half, pl.multiple_of(index * BIG, BIG), pl.multiple_of(start + index * BIG, SUB), BIG, row, None)
                return inner

            lax.fori_loop(0, full_steps, step, 0)
            for count in range(BIG // SUB):

                @pl.when(rest_subs == count)
                def _():
                    key = pl.multiple_of(full_steps * BIG, BIG)
                    block(half, key, pl.multiple_of(start + full_steps * BIG, SUB), (count + 1) * SUB, row, bound)

        def score_pass(half, inner):
            row = geometry(half)[4]
            qt_ref[half] = q_ref[pl.ds(row, tile), :].T
            gt_ref[half] = g_ref[pl.ds(row, tile), :].T
            m_ref[half] = jnp.full((8, tile), MASK_VALUE, jnp.float32)
            sweep(half, score_block)
            return inner

        def value_pass(half, inner):
            row = geometry(half)[4]
            m_ref[half] = wide(jnp.max(m_ref[half], axis=0, keepdims=True) * log2_scale)
            l_ref[half] = jnp.zeros((8, tile), jnp.float32)
            ot_ref[half] = jnp.zeros((head_dim, tile), jnp.float32)
            sweep(half, value_block)
            row_sum = jnp.sum(l_ref[half], axis=0, keepdims=True)
            out = (ot_ref[half] / row_sum).astype(jnp.bfloat16)
            o_ref[pl.ds(row, tile), :] = out.T
            m_ref[half] += wide(jnp.log2(row_sum))
            l_ref[half] = wide(jnp.sum(out.astype(jnp.float32) * gt_ref[half].astype(jnp.float32), axis=0, keepdims=True))
            return inner

        def grad_pass(half, inner):
            row = geometry(half)[4]
            dqt_ref[half] = jnp.zeros((head_dim, tile), jnp.float32)
            sweep(half, grad_block)
            dq_ref[pl.ds(row, tile), :] = (dqt_ref[half] * scale).astype(jnp.bfloat16).T
            return inner

        for one_pass in (score_pass, value_pass, grad_pass):
            lax.fori_loop(0, 2, one_pass, 0)
        return carry

    lax.fori_loop(0, half_len // POS, pair, 0)


def _work_shapes(seq_len, head_dim, tile):
    strip_rows = (seq_len // SUB + 3) * SUB
    return [
        pltpu.VMEM((head_dim, seq_len), jnp.bfloat16),
        pltpu.VMEM((head_dim, seq_len), jnp.bfloat16),
        pltpu.VMEM((strip_rows, tile), jnp.float32),
        pltpu.VMEM((2, head_dim, tile), jnp.bfloat16),
        pltpu.VMEM((2, head_dim, tile), jnp.bfloat16),
        pltpu.VMEM((2, head_dim, tile), jnp.float32),
        pltpu.VMEM((2, head_dim, tile), jnp.float32),
        pltpu.VMEM((2, 8, tile), jnp.float32),
        pltpu.VMEM((2, 8, tile), jnp.float32),
    ]


def _kernel(ctx_size, heads, aliased, q_ref, g_ref, kv_hbm, *rest):
    if aliased:
        rest = rest[2:]
    o_ref, dq_ref, dkv_hbm, k_ref, v_ref, dk_ref, dv_ref, load_sem, store_sem, *work = rest
    step = pl.program_id(0)
    half_len = kv_hbm.shape[3] // 2
    last_piece = 2 * ctx_size - 1

    def pieces(make):
        def each(dev, carry):
            for half in range(2):
                piece = dev + half * (last_piece - 2 * dev)
                there = pl.ds(half * half_len, half_len)
                here = pl.ds(pl.multiple_of(piece * half_len, half_len), half_len)
                for which in range(2):
                    make(dev, which, there, here)
            return carry

        lax.fori_loop(0, ctx_size, each, 0)

    def load(dev, which, there, here):
        pltpu.make_async_copy(kv_hbm.at[dev, step, which, there, :], (k_ref, v_ref)[which].at[here, :], load_sem.at[which]).start()

    def store(dev, which, there, here):
        pltpu.make_async_copy((dk_ref, dv_ref)[which].at[here, :], dkv_hbm.at[dev, step, which, there, :], store_sem.at[which]).start()

    def wait_for(ref, sem):
        pltpu.make_async_copy(ref, ref, sem).wait()

    pieces(load)
    wait_for(k_ref, load_sem.at[0])
    wait_for(v_ref, load_sem.at[1])
    _attention_sequence(lax.axis_index("ctx"), ctx_size, heads, q_ref, g_ref, k_ref, v_ref, o_ref, dq_ref, dk_ref, dv_ref, work)
    pieces(store)
    wait_for(dk_ref, store_sem.at[0])
    wait_for(dv_ref, store_sem.at[1])


def solution(mesh):
    ctx_size = mesh.shape["ctx"]
    block_spec = P("data", "ctx", None, None)

    def local_attention(queries, keys_in, values_in, grad_out):
        batch, shard_len, heads, head_dim = queries.shape
        rows, seq_len, tile = shard_len * heads, shard_len * ctx_size, POS * heads
        group = 2
        q_rows = queries.reshape(batch, rows, head_dim)
        g_rows = grad_out.reshape(batch, rows, head_dim)
        kv_local = jnp.stack([keys_in.reshape(batch, shard_len, head_dim), values_in.reshape(batch, shard_len, head_dim)], axis=1)
        row_shape = jax.ShapeDtypeStruct((batch, rows, head_dim), jnp.bfloat16)
        results = None
        grads = []
        gathered = [lax.all_gather(kv_local[first : first + group], "ctx", axis=0, tiled=False) for first in range(0, batch, group)]
        for part, first in enumerate(range(0, batch, group)):
            row_block = pl.BlockSpec((None, rows, head_dim), lambda step, first=first: (first + step, 0, 0))
            any_spec = pl.BlockSpec(memory_space=pl.ANY)
            operands = [q_rows, g_rows, gathered[part]] + list(results or [])
            out = pl.pallas_call(
                functools.partial(_kernel, ctx_size, heads, results is not None),
                grid=(group,),
                out_shape=[row_shape, row_shape, jax.ShapeDtypeStruct((ctx_size, group, 2, shard_len, head_dim), jnp.float32)],
                in_specs=[row_block, row_block] + [any_spec] * (len(operands) - 2),
                out_specs=[row_block, row_block, any_spec],
                input_output_aliases={3: 0, 4: 1} if results else {},
                scratch_shapes=[
                    pltpu.VMEM((seq_len, head_dim), jnp.bfloat16),
                    pltpu.VMEM((seq_len, head_dim), jnp.bfloat16),
                    pltpu.VMEM((seq_len, head_dim), jnp.float32),
                    pltpu.VMEM((seq_len, head_dim), jnp.float32),
                    pltpu.SemaphoreType.DMA((2,)),
                    pltpu.SemaphoreType.DMA((2,)),
                ]
                + _work_shapes(seq_len, head_dim, tile),
                compiler_params=pltpu.CompilerParams(vmem_limit_bytes=VMEM_BYTES),
                cost_estimate=pl.CostEstimate(flops=2 * 10**10, bytes_accessed=10**8, transcendentals=0),
            )(*operands)
            results = out[:2]
            grads.append(lax.psum_scatter(out[2], "ctx", scatter_dimension=0, tiled=False))
        grad_kv = jnp.concatenate(grads, axis=0)
        grad_k = (grad_kv[:, 0] * head_dim**-0.5).astype(jnp.bfloat16)
        grad_v = grad_kv[:, 1].astype(jnp.bfloat16)
        attn_out = results[0].reshape(queries.shape)
        grad_q = results[1].reshape(queries.shape)
        return attn_out, grad_q, grad_k.reshape(keys_in.shape), grad_v.reshape(values_in.shape)

    return jax.shard_map(local_attention, mesh=mesh, in_specs=(block_spec,) * 4, out_specs=(block_spec,) * 4, check_vma=False)
```

```python
import functools
import math

import jax
import jax.numpy as jnp
from jax import lax
from jax.experimental import pallas as pl
from jax.experimental.pallas import tpu as pltpu
from jax.sharding import PartitionSpec as P

MASK_VALUE = -1e30
BIG = 1024
SUB = 256
POS = 64
VMEM_BYTES = 60 * 2**20


def _dot(lhs, rhs):
    return lax.dot_general(lhs, rhs, (((1,), (0,)), ((), ())), preferred_element_type=jnp.float32)


def _attention_sequence(my_index, ctx_size, heads, q_ref, g_ref, k_ref, v_ref, o_ref, dq_ref, dk_ref, dv_ref, work, between):
    kt_ref, vt_ref, strip, qt_ref, gt_ref, ot_ref, dqt_ref, m_ref, l_ref = work
    seq_len, head_dim = k_ref.shape
    rows = q_ref.shape[0]
    half_len = rows // heads // 2
    tile = POS * heads
    scale = head_dim**-0.5
    log2_scale = scale * math.log2(math.e)
    last_piece = 2 * ctx_size - 1

    def prepare(step, carry):
        span = pl.ds(pl.multiple_of(step * BIG, BIG), BIG)
        kt_ref[:, span] = k_ref[span, :].T
        vt_ref[:, span] = v_ref[span, :].T
        return carry

    lax.fori_loop(0, seq_len // BIG, prepare, 0)

    def wide(row):
        return jnp.broadcast_to(row, (8, tile))

    def fold(block):
        return block.reshape(block.shape[0] // 8, 8, tile)

    def pair(pair_index, carry):
        low_subs = (my_index * half_len + POS * (pair_index + 1) - 1) // SUB + 1

        def geometry(half):
            piece = my_index + half * (last_piece - 2 * my_index)
            bound = piece * half_len + POS * (pair_index + 1)
            full_subs = (bound - 1) // SUB
            row = pl.multiple_of(half * (rows // 2) + pair_index * tile, tile)
            return bound, full_subs // (BIG // SUB), full_subs % (BIG // SUB), half * low_subs * SUB, row

        def score_block(half, key, at, size, row, bound):
            run_max = m_ref[half]
            for sub in range(0, size, SUB):
                scores = _dot(k_ref[pl.ds(key + sub, SUB), :], qt_ref[half])
                if bound is not None and sub + SUB == size:
                    key_pos = key + sub + lax.broadcasted_iota(jnp.int32, (SUB, 1), 0)
                    query_pos = bound - POS + lax.broadcasted_iota(jnp.int32, (1, tile), 1) // heads
                    scores = jnp.where(key_pos <= query_pos, scores, MASK_VALUE)
                strip[pl.ds(at + sub, SUB), :] = scores
                run_max = jnp.maximum(run_max, jnp.max(fold(scores), axis=0))
            m_ref[half] = run_max

        def value_block(half, key, at, size, row, bound):
            run_sum, shift, total = l_ref[half], m_ref[half], None
            for sub in range(0, size, SUB):
                probs = jnp.exp2(fold(strip[pl.ds(at + sub, SUB), :]) * log2_scale - shift[None])
                run_sum = run_sum + jnp.sum(probs, axis=0)
                part = _dot(vt_ref[:, pl.ds(key + sub, SUB)], probs.reshape(SUB, tile).astype(jnp.bfloat16))
                total = part if total is None else total + part
            l_ref[half] = run_sum
            ot_ref[half] += total

        def grad_block(half, key, at, size, row, bound):
            log_sum, d_row, total = m_ref[half], l_ref[half], None
            for sub in range(0, size, SUB):
                span = pl.ds(key + sub, SUB)
                dprobs = _dot(v_ref[span, :], gt_ref[half])
                probs = jnp.exp2(fold(strip[pl.ds(at + sub, SUB), :]) * log2_scale - log_sum[None])
                dscores = probs * (fold(dprobs) - d_row[None])
                probs = probs.reshape(SUB, tile).astype(jnp.bfloat16)
                dscores = dscores.reshape(SUB, tile).astype(jnp.bfloat16)
                dv_ref[span, :] += _dot(probs, g_ref[pl.ds(row, tile), :])
                dk_ref[span, :] += _dot(dscores, q_ref[pl.ds(row, tile), :])
                part = _dot(kt_ref[:, span], dscores)
                total = part if total is None else total + part
            dqt_ref[half] += total

        def sweep(half, block):
            bound, full_steps, rest_subs, start, row = geometry(half)

            def step(index, inner):
                block(half, pl.multiple_of(index * BIG, BIG), pl.multiple_of(start + index * BIG, SUB), BIG, row, None)
                return inner

            lax.fori_loop(0, full_steps, step, 0)
            for count in range(BIG // SUB):

                @pl.when(rest_subs == count)
                def _():
                    key = pl.multiple_of(full_steps * BIG, BIG)
                    block(half, key, pl.multiple_of(start + full_steps * BIG, SUB), (count + 1) * SUB, row, bound)

        def score_pass(half, inner):
            row = geometry(half)[4]
            qt_ref[half] = q_ref[pl.ds(row, tile), :].T
            gt_ref[half] = g_ref[pl.ds(row, tile), :].T
            m_ref[half] = jnp.full((8, tile), MASK_VALUE, jnp.float32)
            sweep(half, score_block)
            return inner

        def value_pass(half, inner):
            row = geometry(half)[4]
            m_ref[half] = wide(jnp.max(m_ref[half], axis=0, keepdims=True) * log2_scale)
            l_ref[half] = jnp.zeros((8, tile), jnp.float32)
            ot_ref[half] = jnp.zeros((head_dim, tile), jnp.float32)
            sweep(half, value_block)
            row_sum = jnp.sum(l_ref[half], axis=0, keepdims=True)
            out = (ot_ref[half] / row_sum).astype(jnp.bfloat16)
            o_ref[pl.ds(row, tile), :] = out.T
            m_ref[half] += wide(jnp.log2(row_sum))
            l_ref[half] = wide(jnp.sum(out.astype(jnp.float32) * gt_ref[half].astype(jnp.float32), axis=0, keepdims=True))
            return inner

        def grad_pass(half, inner):
            row = geometry(half)[4]
            dqt_ref[half] = jnp.zeros((head_dim, tile), jnp.float32)
            sweep(half, grad_block)
            dq_ref[pl.ds(row, tile), :] = (dqt_ref[half] * scale).astype(jnp.bfloat16).T
            return inner

        for pass_index, one_pass in enumerate((score_pass, value_pass, grad_pass)):
            between(pair_index, pass_index)
            lax.fori_loop(0, 2, one_pass, 0)
        return carry

    lax.fori_loop(0, half_len // POS, pair, 0)


def _work_shapes(seq_len, head_dim, tile):
    strip_rows = (seq_len // SUB + 3) * SUB
    return [
        pltpu.VMEM((head_dim, seq_len), jnp.bfloat16),
        pltpu.VMEM((head_dim, seq_len), jnp.bfloat16),
        pltpu.VMEM((strip_rows, tile), jnp.float32),
        pltpu.VMEM((2, head_dim, tile), jnp.bfloat16),
        pltpu.VMEM((2, head_dim, tile), jnp.bfloat16),
        pltpu.VMEM((2, head_dim, tile), jnp.float32),
        pltpu.VMEM((2, head_dim, tile), jnp.float32),
        pltpu.VMEM((2, 8, tile), jnp.float32),
        pltpu.VMEM((2, 8, tile), jnp.float32),
    ]


MESH = pl.DeviceIdType.MESH
STEPS = 9

GATHER_AT = {1: (-1, 1, 2, 3, 5), 2: (3, 5, 6, 8, 10)}


def _gather_at(seq):
    if seq in GATHER_AT:
        return GATHER_AT[seq]
    start = STEPS * (seq - 2) - 1
    return tuple(start + gap for gap in (0, 3, 6, 9, 12))


def _kernel(ctx_size, heads, q_hbm, g_hbm, k_hbm, v_hbm, o_hbm, dq_hbm, dk_hbm, dv_hbm, kv_all, *scratch):
    (
        qg_buf,
        od_buf,
        kv_buf,
        acc,
        part,
        ring_in,
        out_buf,
        gather_recv,
        gather_send,
        gather_peer_recv,
        gather_peer_send,
        load_sem,
        qg_sem,
        od_sem,
        peer_recv,
        peer_send,
        ring_recv,
        ring_send,
        out_sem,
        peer_credit,
        side_credit,
        *work,
    ) = scratch
    batch, shard_len, head_dim = k_hbm.shape
    half_len = shard_len // 2
    chips = ctx_size // 2
    last_piece = 2 * ctx_size - 1
    me = lax.axis_index("ctx")
    chip, core = me // 2, me % 2

    def device(which_chip, which_core):
        return lax.rem(which_chip + 2 * chips, chips) * 2 + which_core

    peer = device(chip, 1 - core)
    sides = (device(chip + 1, core), device(chip - 1, core))

    def remote(src, dst, send_sem, recv_sem, target):
        return pltpu.make_async_remote_copy(
            src_ref=src, dst_ref=dst, send_sem=send_sem, recv_sem=recv_sem, device_id={"ctx": target}, device_id_type=MESH
        )

    def wait_recv(ref, sem, target):
        remote(ref, ref, sem, sem, target).wait_recv()

    def wait_send(ref, sem, target):
        remote(ref, ref, sem, sem, target).wait_send()

    def wait_local(ref, sem):
        pltpu.make_async_copy(ref, ref, sem).wait()

    def gather_send_own(seq):
        targets = [(sides[way], gather_send.at[way, seq], gather_recv.at[way, seq, 0]) for way in range(2)]
        targets.append((peer, gather_peer_send.at[seq], gather_peer_recv.at[seq]))
        for target, send_sem, recv_sem in targets:
            for which, source in enumerate((k_hbm, v_hbm)):
                remote(source.at[seq], kv_all.at[seq, 2 * me + which], send_sem, recv_sem, target).start()

    def gather_arrival(seq, hop):
        far = []
        for way in range(2):
            origin = device(chip - hop if way == 0 else chip + hop, core)
            units = pl.ds(2 * origin, 2) if hop < 4 else pl.ds(2 * origin + way, 1)
            block = kv_all.at[seq, units]
            wait_recv(block, gather_recv.at[way, seq, hop - 1], sides[way])
            if hop < 4:
                onward = block if hop < 3 else kv_all.at[seq, pl.ds(2 * origin + way, 1)]
                remote(onward, onward, gather_send.at[way, seq], gather_recv.at[way, seq, hop], sides[way]).start()
                far.append(block)
            elif way == 1:
                far.append(kv_all.at[seq, pl.ds(2 * origin, 2)])
        for block in far:
            remote(block, block, gather_peer_send.at[seq], gather_peer_recv.at[seq], peer).start()

    def load_keys(seq):
        wait_recv(kv_all.at[seq, pl.ds(0, ctx_size)], gather_peer_recv.at[seq], peer)
        slot = seq % 2

        def each(dev, carry):
            for half in range(2):
                piece = dev + half * (last_piece - 2 * dev)
                there = pl.ds(half * half_len, half_len)
                here = pl.ds(pl.multiple_of(piece * half_len, half_len), half_len)
                for which, own in enumerate((k_hbm, v_hbm)):
                    target = kv_buf.at[slot, which, here, :]

                    @pl.when(dev == me)
                    def _():
                        pltpu.make_async_copy(own.at[seq, there, :], target, load_sem.at[slot]).start()

                    @pl.when(dev != me)
                    def _():
                        pltpu.make_async_copy(kv_all.at[seq, 2 * dev + which, there, :], target, load_sem.at[slot]).start()

            return carry

        lax.fori_loop(0, ctx_size, each, 0)

    def piece_rows(dev, half):
        piece = dev + half * (last_piece - 2 * dev)
        return pl.ds(pl.multiple_of(piece * half_len, half_len), half_len)

    def reduce_peer_send(seq):
        slot = seq % 2

        @pl.when(seq >= 2)
        def _():
            pl.semaphore_wait(peer_credit, 1)

        def each(where, carry):
            for half in range(2):
                for which in range(2):
                    remote(
                        acc.at[which, piece_rows(2 * where + 1 - core, half), :],
                        part.at[slot, 2 * where + which, pl.ds(half * half_len, half_len), :],
                        peer_send.at[slot],
                        peer_recv.at[slot],
                        peer,
                    ).start()
            return carry

        lax.fori_loop(0, chips, each, 0)

    def clear_grads():
        def each(step, carry):
            for which in range(2):
                acc[which, pl.ds(pl.multiple_of(step * SUB, SUB), SUB), :] = jnp.zeros((SUB, head_dim), jnp.float32)
            return carry

        lax.fori_loop(0, acc.shape[1] // SUB, each, 0)

    def ring_chunk(slot, step, way):
        target = lax.rem(chip + (5 - step if way == 0 else step - 5) + chips, chips)
        return part.at[slot, pl.ds(2 * target, 2)] if step > 1 else part.at[slot, pl.ds(2 * target + way, 1)]

    def ring_landing(slot, step, way):
        return ring_in.at[slot, way, pl.ds(2 * (step - 1), 2)] if step > 1 else ring_in.at[slot, way, pl.ds(way, 1)]

    def ring_start(slot, step):
        for way in range(2):
            remote(
                ring_chunk(slot, step, way),
                ring_landing(slot, step, way),
                ring_send.at[slot, way],
                ring_recv.at[slot, way, step - 1],
                sides[way],
            ).start()

    def reduce_begin(seq):
        slot = seq % 2
        wait_send(part.at[slot], peer_send.at[slot], peer)
        wait_recv(part.at[slot], peer_recv.at[slot], peer)

        def each(where, carry):
            for half in range(2):
                for which in range(2):
                    place = pl.ds(half * half_len, half_len)
                    part[slot, 2 * where + which, place, :] += acc[which, piece_rows(2 * where + core, half), :]
            return carry

        lax.fori_loop(0, chips, each, 0)
        clear_grads()

        @pl.when(seq >= 2)
        def _():
            for way in range(2):
                pl.semaphore_wait(side_credit.at[way], 1)

        ring_start(slot, 1)

    def reduce_step(seq, step):
        slot = seq % 2
        for way in range(2):
            landing = ring_landing(slot, step - 1, way)
            wait_recv(landing, ring_recv.at[slot, way, step - 2], sides[way])
            chunk = ring_chunk(slot, step, way)
            for unit in range(2) if step > 2 else (way,):
                chunk[unit] += landing[unit if step > 2 else 0]
        ring_start(slot, step)

    def reduce_end(seq):
        slot = seq % 2

        @pl.when(seq >= 2)
        def _():
            wait_local(out_buf.at[slot], out_sem.at[slot])

        for way in range(2):
            wait_recv(ring_landing(slot, 4, way), ring_recv.at[slot, way, 3], sides[way])
        for which in range(2):
            total = part[slot, 2 * chip + which] + ring_in[slot, 0, 6 + which] + ring_in[slot, 1, 6 + which]
            out_buf[slot, which] = (total * (head_dim**-0.5) if which == 0 else total).astype(jnp.bfloat16)
        for which, target in enumerate((dk_hbm, dv_hbm)):
            pltpu.make_async_copy(out_buf.at[slot, which], target.at[seq], out_sem.at[slot]).start()
        for way in range(2):
            wait_send(ring_in.at[slot, way, pl.ds(0, 7)], ring_send.at[slot, way], sides[way])

        @pl.when(seq + 2 < batch)
        def _():
            pl.semaphore_signal(peer_credit, 1, device_id={"ctx": peer}, device_id_type=MESH)
            for way in range(2):
                pl.semaphore_signal(side_credit.at[1 - way], 1, device_id={"ctx": sides[way]}, device_id_type=MESH)

    def load_rows(seq):
        for which, source in enumerate((q_hbm, g_hbm)):
            pltpu.make_async_copy(source.at[seq], qg_buf.at[seq % 2, which], qg_sem.at[seq % 2]).start()

    load_rows(0)
    clear_grads()
    barrier = pltpu.get_barrier_semaphore()
    for target in (*sides, peer):
        pl.semaphore_signal(barrier, 1, device_id={"ctx": target}, device_id_type=MESH)
    pl.semaphore_wait(barrier, 3)

    gather_send_own(0)
    for hop in range(1, 4):
        gather_arrival(0, hop)
    gather_send_own(1)
    gather_arrival(0, 4)
    load_keys(0)

    events = [[] for _ in range(STEPS)]
    for seq in range(1, batch):
        for hop, at in enumerate(_gather_at(seq)):
            if at >= 0:
                events[at % STEPS].append((at // STEPS, functools.partial(gather_send_own, seq) if hop == 0 else functools.partial(gather_arrival, seq, hop)))

    def sequence(seq, carry):
        slot = seq % 2
        wait_local(kv_buf.at[slot], load_sem.at[slot])
        wait_local(qg_buf.at[slot], qg_sem.at[slot])

        @pl.when(seq + 1 < batch)
        def _():
            load_rows(seq + 1)

        def between(pair_index, pass_index):
            for pair in range(STEPS // 3):
                step = 3 * pair + pass_index

                @pl.when(pair_index == pair)
                def _():
                    if step == 0:

                        @pl.when(seq >= 1)
                        def _():
                            reduce_peer_send(seq - 1)

                        @pl.when(seq >= 2)
                        def _():
                            reduce_step(seq - 2, 4)

                    if step == 1:

                        @pl.when(seq >= 1)
                        def _():
                            wait_local(od_buf, od_sem)

                    if step in (2, 4, 6):

                        @pl.when(seq >= 1)
                        def _():
                            if step == 2:
                                reduce_begin(seq - 1)
                            else:
                                reduce_step(seq - 1, step // 2)

                    if step == 3:

                        @pl.when(seq >= 2)
                        def _():
                            reduce_end(seq - 2)

                    for when, event in events[step]:

                        @pl.when(seq == when)
                        def _():
                            event()

                    if step == 6:

                        @pl.when(seq + 1 < batch)
                        def _():
                            load_keys(seq + 1)

        _attention_sequence(
            me,
            ctx_size,
            heads,
            qg_buf.at[slot, 0],
            qg_buf.at[slot, 1],
            kv_buf.at[slot, 0],
            kv_buf.at[slot, 1],
            od_buf.at[0],
            od_buf.at[1],
            acc.at[0],
            acc.at[1],
            work,
            between,
        )
        for which, target in enumerate((o_hbm, dq_hbm)):
            pltpu.make_async_copy(od_buf.at[which], target.at[seq], od_sem).start()
        return carry

    lax.fori_loop(0, batch, sequence, 0)

    last = batch - 1
    reduce_peer_send(last)
    reduce_step(last - 1, 4)
    reduce_begin(last)
    reduce_end(last - 1)
    for step in range(2, 5):
        reduce_step(last, step)
    reduce_end(last)
    wait_local(od_buf, od_sem)
    for slot in range(2):
        wait_local(out_buf.at[slot], out_sem.at[slot])

    def drain(seq, carry):
        for way in range(2):
            wait_send(kv_all.at[seq, pl.ds(0, 7)], gather_send.at[way, seq], sides[way])
        wait_send(kv_all.at[seq, pl.ds(0, ctx_size)], gather_peer_send.at[seq], peer)
        return carry

    lax.fori_loop(0, batch, drain, 0)


def solution(mesh):
    ctx_size = mesh.shape["ctx"]
    block_spec = P("data", "ctx", None, None)

    def local_attention(queries, keys_in, values_in, grad_out):
        batch, shard_len, heads, head_dim = queries.shape
        rows, seq_len, tile = shard_len * heads, shard_len * ctx_size, POS * heads
        row_shape = jax.ShapeDtypeStruct((batch, rows, head_dim), jnp.bfloat16)
        shard_shape = jax.ShapeDtypeStruct((batch, shard_len, head_dim), jnp.bfloat16)
        dma, regular = pltpu.SemaphoreType.DMA, pltpu.SemaphoreType.REGULAR
        attn_out, grad_q, grad_k, grad_v, _ = pl.pallas_call(
            functools.partial(_kernel, ctx_size, heads),
            out_shape=[
                row_shape,
                row_shape,
                shard_shape,
                shard_shape,
                jax.ShapeDtypeStruct((batch, 2 * ctx_size, shard_len, head_dim), jnp.bfloat16),
            ],
            in_specs=[pl.BlockSpec(memory_space=pl.ANY)] * 4,
            out_specs=[pl.BlockSpec(memory_space=pl.ANY)] * 5,
            scratch_shapes=[
                pltpu.VMEM((2, 2, rows, head_dim), jnp.bfloat16),
                pltpu.VMEM((2, rows, head_dim), jnp.bfloat16),
                pltpu.VMEM((2, 2, seq_len, head_dim), jnp.bfloat16),
                pltpu.VMEM((2, seq_len, head_dim), jnp.float32),
                pltpu.VMEM((2, ctx_size, shard_len, head_dim), jnp.float32),
                pltpu.VMEM((2, 2, 8, shard_len, head_dim), jnp.float32),
                pltpu.VMEM((2, 2, shard_len, head_dim), jnp.bfloat16),
                dma((2, batch, 4)),
                dma((2, batch)),
                dma((batch,)),
                dma((batch,)),
                dma((2,)),
                dma((2,)),
                dma,
                dma((2,)),
                dma((2,)),
                dma((2, 2, 4)),
                dma((2, 2)),
                dma((2,)),
                regular,
                regular((2,)),
            ]
            + _work_shapes(seq_len, head_dim, tile),
            compiler_params=pltpu.CompilerParams(vmem_limit_bytes=VMEM_BYTES, collective_id=0, has_side_effects=True),
            cost_estimate=pl.CostEstimate(flops=10**11, bytes_accessed=10**8, transcendentals=0),
        )(
            queries.reshape(batch, rows, head_dim),
            grad_out.reshape(batch, rows, head_dim),
            keys_in.reshape(batch, shard_len, head_dim),
            values_in.reshape(batch, shard_len, head_dim),
        )
        return attn_out.reshape(queries.shape), grad_q.reshape(queries.shape), grad_k.reshape(keys_in.shape), grad_v.reshape(values_in.shape)

    return jax.shard_map(local_attention, mesh=mesh, in_specs=(block_spec,) * 4, out_specs=(block_spec,) * 4, check_vma=False)
```

```python
import functools
import math

import jax
import jax.numpy as jnp
from jax import lax
from jax.experimental import pallas as pl
from jax.experimental.pallas import tpu as pltpu
from jax.sharding import PartitionSpec as P

MASK_VALUE = -1e30
BIG = 1024
SUB = 256
POS = 64
VMEM_BYTES = 60 * 2**20


def _dot_first(lhs, rhs):
    return lax.dot_general(lhs, rhs, (((0,), (0,)), ((), ())), preferred_element_type=jnp.float32)


def _dot(lhs, rhs):
    return lax.dot_general(lhs, rhs, (((1,), (0,)), ((), ())), preferred_element_type=jnp.float32)


def _attention_sequence(my_index, ctx_size, heads, q_ref, g_ref, k_ref, v_ref, o_ref, dq_ref, dk_ref, dv_ref, work, between):
    strip, recent, qt_ref, gt_ref, ot_ref, dqt_ref, max_ref, used_max_ref, sum_ref = work
    head_dim = k_ref.shape[1]
    rows = q_ref.shape[0]
    half_len = rows // heads // 2
    tile = POS * heads
    subs = BIG // SUB
    scale = head_dim**-0.5
    log2_scale = scale * math.log2(math.e)
    last_piece = 2 * ctx_size - 1

    def wide(row):
        return jnp.broadcast_to(row, (8, tile))

    def top(partial):
        return wide(jnp.max(partial, axis=0, keepdims=True)) * log2_scale

    def fold(block):
        return block.reshape(block.shape[0] // 8, 8, tile)

    def add(total, part):
        return part if total is None else total + part

    def pair(pair_index, carry):
        low_subs = (my_index * half_len + POS * (pair_index + 1) - 1) // SUB + 1

        def geometry(half):
            piece = my_index + half * (last_piece - 2 * my_index)
            bound = piece * half_len + POS * (pair_index + 1)
            full_subs = (bound - 1) // SUB
            row = pl.multiple_of(half * (rows // 2) + pair_index * tile, tile)
            return bound, full_subs // subs, full_subs % subs, half * low_subs * SUB, row

        def score(half, key, at, sub, partial, bound=None):
            scores = _dot(k_ref[pl.ds(key, SUB), :], qt_ref[half])
            if bound is not None:
                key_pos = key + lax.broadcasted_iota(jnp.int32, (SUB, 1), 0)
                query_pos = bound - POS + lax.broadcasted_iota(jnp.int32, (1, tile), 1) // heads
                scores = jnp.where(key_pos <= query_pos, scores, MASK_VALUE)
            strip[pl.ds(at, SUB), :] = scores
            recent[sub * SUB : (sub + 1) * SUB, :] = scores
            return jnp.maximum(partial, jnp.max(fold(scores), axis=0))

        def value(key, sub, shift, run_sum, total):
            probs = jnp.exp2(fold(recent[sub * SUB : (sub + 1) * SUB, :]) * log2_scale - shift[None])
            part = _dot_first(v_ref[pl.ds(key, SUB), :], probs.reshape(SUB, tile).astype(jnp.bfloat16))
            return run_sum + jnp.sum(probs, axis=0), add(total, part)

        def rescaled(half, total, decay):
            ot_ref[half] = (fold(ot_ref[half]) * decay[None]).reshape(head_dim, tile) + total

        def forward_pass(half, inner):
            bound, full_steps, rest_subs, start, row = geometry(half)
            qt_ref[half] = q_ref[pl.ds(row, tile), :].T
            gt_ref[half] = g_ref[pl.ds(row, tile), :].T
            lowest = jnp.full((8, tile), MASK_VALUE, jnp.float32)
            for count in range(subs):

                @pl.when(rest_subs == count)
                def _():
                    key, at = pl.multiple_of(full_steps * BIG, BIG), pl.multiple_of(start, SUB)
                    partial = lowest
                    for sub in range(count + 1):
                        partial = score(half, key + sub * SUB, at + sub * SUB, sub, partial, bound if sub == count else None)
                    shift = top(partial)
                    run_sum, total, ahead = jnp.zeros((8, tile), jnp.float32), None, partial
                    for sub in range(subs):
                        if sub <= count:
                            run_sum, total = value(key + sub * SUB, sub, shift, run_sum, total)
                        ahead = score(half, sub * SUB, at + (count + 1 + sub) * SUB, sub, ahead)
                    ot_ref[half] = total
                    sum_ref[half] = run_sum
                    used_max_ref[half] = shift
                    max_ref[half] = jnp.where(full_steps > 0, top(ahead), shift)

            def step(index, last):
                key = pl.multiple_of((index - 1) * BIG, BIG)
                at = pl.multiple_of(start + (rest_subs + 1) * SUB + index * BIG, SUB)
                shift = max_ref[half]
                decay = jnp.exp2(used_max_ref[half] - shift)
                run_sum, total, partial = sum_ref[half] * decay, None, lowest
                for sub in range(subs):
                    run_sum, total = value(key + sub * SUB, sub, shift, run_sum, total)
                    if not last:
                        partial = score(half, key + BIG + sub * SUB, at + sub * SUB, sub, partial)
                sum_ref[half] = run_sum
                rescaled(half, total, decay)
                used_max_ref[half] = shift
                if not last:
                    max_ref[half] = jnp.maximum(shift, top(partial))

            def inner_step(index, carry):
                step(index, False)
                return carry

            lax.fori_loop(1, full_steps, inner_step, 0)

            @pl.when(full_steps > 0)
            def _():
                step(full_steps, True)

            row_sum = jnp.sum(sum_ref[half], axis=0, keepdims=True)
            out = (ot_ref[half] / row_sum).astype(jnp.bfloat16)
            o_ref[pl.ds(row, tile), :] = out.T
            max_ref[half] = used_max_ref[half] + wide(jnp.log2(row_sum))
            sum_ref[half] = wide(jnp.sum(out.astype(jnp.float32) * gt_ref[half].astype(jnp.float32), axis=0, keepdims=True))
            return inner

        def grad(half, key, at, size, row):
            log_sum, d_row, total = max_ref[half], sum_ref[half], None
            for sub in range(0, size, SUB):
                span = pl.ds(key + sub, SUB)
                dprobs = _dot(v_ref[span, :], gt_ref[half])
                probs = jnp.exp2(fold(strip[pl.ds(at + sub, SUB), :]) * log2_scale - log_sum[None])
                dscores = probs * (fold(dprobs) - d_row[None])
                probs = probs.reshape(SUB, tile).astype(jnp.bfloat16)
                dscores = dscores.reshape(SUB, tile).astype(jnp.bfloat16)
                dv_ref[span, :] += _dot(probs, g_ref[pl.ds(row, tile), :])
                dk_ref[span, :] += _dot(dscores, q_ref[pl.ds(row, tile), :])
                total = add(total, _dot_first(k_ref[span, :], dscores))
            dqt_ref[half] += total

        def backward_pass(half, inner):
            bound, full_steps, rest_subs, start, row = geometry(half)
            main = start + (rest_subs + 1) * SUB
            dqt_ref[half] = jnp.zeros((head_dim, tile), jnp.float32)

            def step(index, carry):
                key = pl.multiple_of(index * 2 * BIG, BIG)
                grad(half, key, pl.multiple_of(main + key, SUB), 2 * BIG, row)
                return carry

            lax.fori_loop(0, full_steps // 2, step, 0)

            @pl.when(full_steps % 2 == 1)
            def _():
                key = pl.multiple_of((full_steps - 1) * BIG, BIG)
                grad(half, key, pl.multiple_of(main + key, SUB), BIG, row)

            for count in range(subs):

                @pl.when(rest_subs == count)
                def _():
                    grad(half, pl.multiple_of(full_steps * BIG, BIG), pl.multiple_of(start, SUB), (count + 1) * SUB, row)

            dq_ref[pl.ds(row, tile), :] = (dqt_ref[half] * scale).astype(jnp.bfloat16).T
            return inner

        for pass_index, one_pass in enumerate((forward_pass, backward_pass)):
            between(pair_index, pass_index)
            lax.fori_loop(0, 2, one_pass, 0)
        return carry

    lax.fori_loop(0, half_len // POS, pair, 0)


def _work_shapes(seq_len, head_dim, tile):
    strip_rows = (seq_len // SUB + 3 + BIG // SUB) * SUB
    return [
        pltpu.VMEM((strip_rows, tile), jnp.float32),
        pltpu.VMEM((BIG, tile), jnp.float32),
        pltpu.VMEM((2, head_dim, tile), jnp.bfloat16),
        pltpu.VMEM((2, head_dim, tile), jnp.bfloat16),
        pltpu.VMEM((2, head_dim, tile), jnp.float32),
        pltpu.VMEM((2, head_dim, tile), jnp.float32),
        pltpu.VMEM((2, 8, tile), jnp.float32),
        pltpu.VMEM((2, 8, tile), jnp.float32),
        pltpu.VMEM((2, 8, tile), jnp.float32),
    ]


MESH = pl.DeviceIdType.MESH
SLOTS = 6

GATHER_AT = {1: (-1, 1, 3, 4, 5), 2: (0, 2, 4, 7, 9), 3: (1, 5, 8, 10, 13), 4: (11, 14, 17, 18, 21)}


def _gather_at(seq):
    if seq in GATHER_AT:
        return GATHER_AT[seq]
    return tuple(SLOTS * (seq - 2) + gap for gap in (2, 4, 6, 8, 10))


def _kernel(ctx_size, heads, q_hbm, g_hbm, k_hbm, v_hbm, o_hbm, dq_hbm, dk_hbm, dv_hbm, kv_all, *scratch):
    (
        qg_buf,
        od_buf,
        kv_buf,
        acc,
        part,
        ring_in,
        out_buf,
        gather_recv,
        gather_send,
        gather_peer_recv,
        gather_peer_send,
        load_sem,
        qg_sem,
        od_sem,
        peer_recv,
        peer_send,
        ring_recv,
        ring_send,
        out_sem,
        peer_credit,
        side_credit,
        *work,
    ) = scratch
    batch, shard_len, head_dim = k_hbm.shape
    half_len = shard_len // 2
    chips = ctx_size // 2
    last_piece = 2 * ctx_size - 1
    me = lax.axis_index("ctx")
    chip, core = me // 2, me % 2

    def device(which_chip, which_core):
        return lax.rem(which_chip + 2 * chips, chips) * 2 + which_core

    peer = device(chip, 1 - core)
    sides = (device(chip + 1, core), device(chip - 1, core))

    def remote(src, dst, send_sem, recv_sem, target):
        return pltpu.make_async_remote_copy(
            src_ref=src, dst_ref=dst, send_sem=send_sem, recv_sem=recv_sem, device_id={"ctx": target}, device_id_type=MESH
        )

    def wait_recv(ref, sem, target):
        remote(ref, ref, sem, sem, target).wait_recv()

    def wait_send(ref, sem, target):
        remote(ref, ref, sem, sem, target).wait_send()

    def wait_local(ref, sem):
        pltpu.make_async_copy(ref, ref, sem).wait()

    def piece_rows(dev, half):
        piece = dev + half * (last_piece - 2 * dev)
        return pl.ds(pl.multiple_of(piece * half_len, half_len), half_len)

    def shard_refs(seq, dev, which):
        if seq == 0:
            return [kv_buf.at[0, which, piece_rows(dev, half), :] for half in range(2)]
        return [kv_all.at[seq, 2 * dev + which]]

    def send_shard(sources, seq, dev, which, targets):
        for target, send_sem, recv_sem in targets:
            for source, place in zip(sources, shard_refs(seq, dev, which)):
                remote(source, place, send_sem, recv_sem, target).start()

    def to_side(way, seq, which, hop):
        return sides[way], gather_send.at[way, seq], gather_recv.at[way, which, seq, hop]

    def to_peer(seq):
        return peer, gather_peer_send.at[seq], gather_peer_recv.at[seq]

    def gather_send_own(seq):
        for which, source in enumerate((k_hbm, v_hbm)):
            sources = [source.at[seq]]
            if seq == 0:
                sources = [source.at[seq, pl.ds(half * half_len, half_len), :] for half in range(2)]
            send_shard(sources, seq, me, which, [to_side(0, seq, which, 0), to_side(1, seq, which, 0), to_peer(seq)])

    def gather_arrival(seq, hop):
        for which in range(2):
            for way in range(2) if hop < 4 else (which,):
                origin = device(chip - hop if way == 0 else chip + hop, core)
                refs = shard_refs(seq, origin, which)
                wait_recv(kv_all.at[0, 0], gather_recv.at[way, which, seq, hop - 1], sides[way])
                onward = [to_side(way, seq, which, hop)] if hop < (4 if way == which else 3) else []
                send_shard(refs, seq, origin, which, onward + [to_peer(seq)])

    def drain(seq, carry):
        for way in range(2):
            wait_send(kv_all.at[0, pl.ds(0, 7)], gather_send.at[way, seq], sides[way])
        wait_send(kv_all.at[0, pl.ds(0, ctx_size)], gather_peer_send.at[seq], peer)
        return carry

    def load_keys(seq):
        wait_recv(kv_all.at[seq, pl.ds(0, ctx_size)], gather_peer_recv.at[seq], peer)
        slot = seq % 2

        def each(dev, carry):
            for half in range(2):
                piece = dev + half * (last_piece - 2 * dev)
                there = pl.ds(half * half_len, half_len)
                here = pl.ds(pl.multiple_of(piece * half_len, half_len), half_len)
                for which, own in enumerate((k_hbm, v_hbm)):
                    target = kv_buf.at[slot, which, here, :]

                    @pl.when(dev == me)
                    def _():
                        pltpu.make_async_copy(own.at[seq, there, :], target, load_sem.at[slot]).start()

                    @pl.when(dev != me)
                    def _():
                        pltpu.make_async_copy(kv_all.at[seq, 2 * dev + which, there, :], target, load_sem.at[slot]).start()

            return carry

        lax.fori_loop(0, ctx_size, each, 0)

    chunk_order = (chips // 2, chips // 2 - 1, chips // 2 + 1, chips // 2 - 2, chips // 2 + 2, 1, chips - 1, 0)

    def chunk_chip(offset):
        return lax.rem(chip + offset, chips)

    def reduce_peer_send(seq):
        slot = seq % 2

        @pl.when(seq >= 2)
        def _():
            pl.semaphore_wait(peer_credit, 1)

        for index, offset in enumerate(chunk_order):
            where = chunk_chip(offset)
            for half in range(2):
                for which in range(2):
                    remote(
                        acc.at[which, piece_rows(2 * where + 1 - core, half), :],
                        part.at[slot, 2 * where + which, pl.ds(half * half_len, half_len), :],
                        peer_send.at[slot],
                        peer_recv.at[slot, index],
                        peer,
                    ).start()

    def clear_grads():
        def each(step, carry):
            for which in range(2):
                acc[which, pl.ds(pl.multiple_of(step * SUB, SUB), SUB), :] = jnp.zeros((SUB, head_dim), jnp.float32)
            return carry

        lax.fori_loop(0, acc.shape[1] // SUB, each, 0)

    def ring_chunk(slot, step, way, which):
        return part.at[slot, 2 * chunk_chip(5 - step if way == 0 else chips - 5 + step) + which]

    def ring_send_step(slot, step, way, which):
        remote(
            ring_chunk(slot, step, way, which),
            ring_in.at[slot, way, which, step - 1],
            ring_send.at[slot, way],
            ring_recv.at[slot, way, which, step - 1],
            sides[way],
        ).start()

    def ring_wait(slot, step, way, which):
        wait_recv(ring_in.at[slot, way, which, step - 1], ring_recv.at[slot, way, which, step - 1], sides[way])

    def reduce_begin(seq):
        slot = seq % 2

        @pl.when(seq >= 2)
        def _():
            for way in range(2):
                pl.semaphore_wait(side_credit.at[way], 1)

        for index, offset in enumerate(chunk_order):
            where = chunk_chip(offset)
            wait_recv(part.at[slot, pl.ds(2 * where, 2)], peer_recv.at[slot, index], peer)
            for half in range(2):
                for which in range(2):
                    place = pl.ds(half * half_len, half_len)
                    part[slot, 2 * where + which, place, :] += acc[which, piece_rows(2 * where + core, half), :]
            if index == 0:
                for way in range(2):
                    ring_send_step(slot, 1, way, way)
            elif index < 3:
                ring_send_step(slot, 2, index - 1, 2 - index)
        wait_send(part.at[slot], peer_send.at[slot], peer)
        clear_grads()

    def reduce_step(seq, step, long_chain):
        slot = seq % 2
        for way in range(2):
            which = way if long_chain else 1 - way
            ring_wait(slot, step - 1, way, which)
            ring_chunk(slot, step, way, which)[...] += ring_in[slot, way, which, step - 2]
        for way in range(2):
            ring_send_step(slot, step, way, way if long_chain else 1 - way)

    def reduce_end(seq):
        slot = seq % 2

        @pl.when(seq >= 2)
        def _():
            wait_local(out_buf.at[slot], out_sem.at[slot])

        for which, target in enumerate((dk_hbm, dv_hbm)):
            for way in (1 - which, which):
                ring_wait(slot, 4, way, which)
            total = part[slot, 2 * chip + which] + ring_in[slot, 0, which, 3] + ring_in[slot, 1, which, 3]
            out_buf[slot, which] = (total * (head_dim**-0.5) if which == 0 else total).astype(jnp.bfloat16)
            pltpu.make_async_copy(out_buf.at[slot, which], target.at[seq], out_sem.at[slot]).start()
        for way in range(2):
            wait_send(part.at[slot, pl.ds(0, 7)], ring_send.at[slot, way], sides[way])

        @pl.when(seq + 2 < batch)
        def _():
            pl.semaphore_signal(peer_credit, 1, device_id={"ctx": peer}, device_id_type=MESH)
            for way in range(2):
                pl.semaphore_signal(side_credit.at[1 - way], 1, device_id={"ctx": sides[way]}, device_id_type=MESH)

    def load_rows(seq):
        for which, source in enumerate((q_hbm, g_hbm)):
            pltpu.make_async_copy(source.at[seq], qg_buf.at[seq % 2, which], qg_sem.at[seq % 2]).start()

    load_rows(0)
    clear_grads()
    barrier = pltpu.get_barrier_semaphore()
    for target in (*sides, peer):
        pl.semaphore_signal(barrier, 1, device_id={"ctx": target}, device_id_type=MESH)
    pl.semaphore_wait(barrier, 3)

    gather_send_own(0)
    own_loads = [
        pltpu.make_async_copy(source.at[0, pl.ds(half * half_len, half_len), :], place, load_sem.at[0])
        for which, source in enumerate((k_hbm, v_hbm))
        for half, place in enumerate(shard_refs(0, me, which))
    ]
    for copy in own_loads:
        copy.start()
    for hop in range(1, 4):
        gather_arrival(0, hop)
    gather_send_own(1)
    gather_arrival(0, 4)
    wait_recv(kv_all.at[0, pl.ds(0, ctx_size)], gather_peer_recv.at[0], peer)
    wait_local(kv_all.at[0, pl.ds(0, 2)], load_sem.at[0])

    events = [[] for _ in range(SLOTS)]
    for seq in range(1, batch):
        for hop, at in enumerate(_gather_at(seq)):
            if at >= 0:
                event = functools.partial(gather_arrival, seq, hop) if hop else functools.partial(gather_send_own, seq)
                events[at % SLOTS].append((at // SLOTS, event))

    events[0].append((1, functools.partial(drain, 0, 0)))

    def steps(*which):
        return lambda seq: [reduce_step(seq, *one) for one in which]

    last = batch - 1
    reduce_events = {
        (0, 1): reduce_peer_send,
        (1, 1): reduce_begin,
        (3, 1): steps((2, True), (3, False)),
        (4, 1): steps((3, True)),
        (5, 1): steps((4, False)),
        (0, 2): steps((4, True)),
        (3, 2): reduce_end,
    }
    last_events = {
        (0, 1): reduce_peer_send,
        (1, 1): reduce_begin,
        (2, 1): steps((2, True)),
        (3, 1): steps((3, False), (3, True)),
        (5, 1): steps((4, False), (4, True)),
        (0, 2): reduce_events[0, 2],
        (3, 2): reduce_end,
    }

    def sequence(seq, carry):
        slot = seq % 2

        @pl.when(seq >= 1)
        def _():
            wait_local(kv_buf.at[slot], load_sem.at[slot])

        wait_local(qg_buf.at[slot], qg_sem.at[slot])

        @pl.when(seq >= 2)
        def _():
            wait_local(od_buf.at[slot], od_sem.at[slot])

        @pl.when(seq + 1 < batch)
        def _():
            load_rows(seq + 1)

        def between(pair_index, pass_index):
            for pair in range(SLOTS // 2):
                at = 2 * pair + pass_index

                @pl.when(pair_index == pair)
                def _():
                    for when, event in events[at]:

                        @pl.when(seq == when)
                        def _():
                            event()

                    for lag in (2, 1):
                        usual, final = reduce_events.get((at, lag)), last_events.get((at, lag))
                        if usual and usual is final:

                            @pl.when(seq >= lag)
                            def _():
                                usual(seq - lag)

                        elif usual or final:

                            @pl.when((seq >= lag) & (seq < last))
                            def _():
                                if usual:
                                    usual(seq - lag)

                            @pl.when(seq == last)
                            def _():
                                if final:
                                    final(seq - lag)

                    if at == SLOTS - 1:

                        @pl.when(seq + 1 < batch)
                        def _():
                            load_keys(seq + 1)

        _attention_sequence(
            me,
            ctx_size,
            heads,
            qg_buf.at[slot, 0],
            qg_buf.at[slot, 1],
            kv_buf.at[slot, 0],
            kv_buf.at[slot, 1],
            od_buf.at[slot, 0],
            od_buf.at[slot, 1],
            acc.at[0],
            acc.at[1],
            work,
            between,
        )
        for which, target in enumerate((o_hbm, dq_hbm)):
            pltpu.make_async_copy(od_buf.at[slot, which], target.at[seq], od_sem.at[slot]).start()
        return carry

    lax.fori_loop(0, batch, sequence, 0)

    reduce_peer_send(last)
    reduce_begin(last)
    reduce_step(last, 2, True)
    reduce_end(last - 1)
    for step in range(3, 5):
        reduce_step(last, step, False)
        reduce_step(last, step, True)
    reduce_end(last)
    for slot in range(2):
        wait_local(od_buf.at[slot], od_sem.at[slot])
        wait_local(out_buf.at[slot], out_sem.at[slot])

    lax.fori_loop(1, batch, drain, 0)


def solution(mesh):
    ctx_size = mesh.shape["ctx"]
    block_spec = P("data", "ctx", None, None)

    def local_attention(queries, keys_in, values_in, grad_out):
        batch, shard_len, heads, head_dim = queries.shape
        rows, seq_len, tile = shard_len * heads, shard_len * ctx_size, POS * heads
        row_shape = jax.ShapeDtypeStruct((batch, rows, head_dim), jnp.bfloat16)
        shard_shape = jax.ShapeDtypeStruct((batch, shard_len, head_dim), jnp.bfloat16)
        dma, regular = pltpu.SemaphoreType.DMA, pltpu.SemaphoreType.REGULAR
        attn_out, grad_q, grad_k, grad_v, _ = pl.pallas_call(
            functools.partial(_kernel, ctx_size, heads),
            out_shape=[
                row_shape,
                row_shape,
                shard_shape,
                shard_shape,
                jax.ShapeDtypeStruct((batch, 2 * ctx_size, shard_len, head_dim), jnp.bfloat16),
            ],
            in_specs=[pl.BlockSpec(memory_space=pl.ANY)] * 4,
            out_specs=[pl.BlockSpec(memory_space=pl.ANY)] * 5,
            scratch_shapes=[
                pltpu.VMEM((2, 2, rows, head_dim), jnp.bfloat16),
                pltpu.VMEM((2, 2, rows, head_dim), jnp.bfloat16),
                pltpu.VMEM((2, 2, seq_len, head_dim), jnp.bfloat16),
                pltpu.VMEM((2, seq_len, head_dim), jnp.float32),
                pltpu.VMEM((2, ctx_size, shard_len, head_dim), jnp.float32),
                pltpu.VMEM((2, 2, 2, 4, shard_len, head_dim), jnp.float32),
                pltpu.VMEM((2, 2, shard_len, head_dim), jnp.bfloat16),
                dma((2, 2, batch, 4)),
                dma((2, batch)),
                dma((batch,)),
                dma((batch,)),
                dma((2,)),
                dma((2,)),
                dma((2,)),
                dma((2, ctx_size // 2)),
                dma((2,)),
                dma((2, 2, 2, 4)),
                dma((2, 2)),
                dma((2,)),
                regular,
                regular((2,)),
            ]
            + _work_shapes(seq_len, head_dim, tile),
            compiler_params=pltpu.CompilerParams(vmem_limit_bytes=VMEM_BYTES, collective_id=0, has_side_effects=True),
            cost_estimate=pl.CostEstimate(flops=10**11, bytes_accessed=10**8, transcendentals=0),
        )(
            queries.reshape(batch, rows, head_dim),
            grad_out.reshape(batch, rows, head_dim),
            keys_in.reshape(batch, shard_len, head_dim),
            values_in.reshape(batch, shard_len, head_dim),
        )
        return attn_out.reshape(queries.shape), grad_q.reshape(queries.shape), grad_k.reshape(keys_in.shape), grad_v.reshape(values_in.shape)

    return jax.shard_map(local_attention, mesh=mesh, in_specs=(block_spec,) * 4, out_specs=(block_spec,) * 4, check_vma=False)
```

```python
import functools
import math

import jax
import jax.numpy as jnp
from jax import lax
from jax.experimental import pallas as pl
from jax.experimental.pallas import tpu as pltpu
from jax.sharding import PartitionSpec as P

MASK_VALUE = -1e30
BIG = 1024
SUB = 256
POS = 64
VMEM_BYTES = 60 * 2**20


def _dot_first(lhs, rhs):
    return lax.dot_general(lhs, rhs, (((0,), (0,)), ((), ())), preferred_element_type=jnp.float32)


def _dot(lhs, rhs):
    return lax.dot_general(lhs, rhs, (((1,), (0,)), ((), ())), preferred_element_type=jnp.float32)


def _attention_sequence(my_index, ctx_size, heads, q_ref, g_ref, k_ref, v_ref, o_ref, dq_ref, dk_ref, dv_ref, work, between):
    strip, recent, qt_ref, gt_ref, ot_ref, dqt_ref, max_ref, used_max_ref, sum_ref = work
    head_dim = k_ref.shape[1]
    rows = q_ref.shape[0]
    half_len = rows // heads // 2
    tile = POS * heads
    subs = BIG // SUB
    scale = head_dim**-0.5
    log2_scale = scale * math.log2(math.e)
    last_piece = 2 * ctx_size - 1

    def wide(row):
        return jnp.broadcast_to(row, (8, tile))

    def top(partial):
        return wide(jnp.max(partial, axis=0, keepdims=True)) * log2_scale

    def fold(block):
        return block.reshape(block.shape[0] // 8, 8, tile)

    def add(total, part):
        return part if total is None else total + part

    def pair(pair_index, carry):
        low_subs = (my_index * half_len + POS * (pair_index + 1) - 1) // SUB + 1

        def geometry(half):
            piece = my_index + half * (last_piece - 2 * my_index)
            bound = piece * half_len + POS * (pair_index + 1)
            full_subs = (bound - 1) // SUB
            row = pl.multiple_of(half * (rows // 2) + pair_index * tile, tile)
            return bound, full_subs // subs, full_subs % subs, half * low_subs * SUB, row

        def score(half, key, at, sub, partial, bound=None, into=0):
            scores = _dot(k_ref[pl.ds(key, SUB), :], qt_ref[half])
            if bound is not None:
                key_pos = key + lax.broadcasted_iota(jnp.int32, (SUB, 1), 0)
                query_pos = bound - POS + lax.broadcasted_iota(jnp.int32, (1, tile), 1) // heads
                scores = jnp.where(key_pos <= query_pos, scores, MASK_VALUE)
            strip[pl.ds(at, SUB), :] = scores
            recent[into, sub * SUB : (sub + 1) * SUB, :] = scores
            return jnp.maximum(partial, jnp.max(fold(scores), axis=0))

        def weights(sub, shift, source=0):
            return jnp.exp2(fold(recent[source, sub * SUB : (sub + 1) * SUB, :]) * log2_scale - shift[None])

        def value(key, probs, total):
            return add(total, _dot_first(v_ref[pl.ds(key, SUB), :], probs.reshape(SUB, tile).astype(jnp.bfloat16)))

        def rescaled(half, total, decay):
            ot_ref[half] = (fold(ot_ref[half]) * decay[None]).reshape(head_dim, tile) + total

        def forward_pass(half, inner):
            bound, full_steps, rest_subs, start, row = geometry(half)
            lowest = jnp.full((8, tile), MASK_VALUE, jnp.float32)
            for count in range(subs):

                @pl.when(rest_subs == count)
                def _():
                    key, at = pl.multiple_of(full_steps * BIG, BIG), pl.multiple_of(start, SUB)
                    partial = lowest
                    for sub in range(count + 1):
                        partial = score(half, key + sub * SUB, at + sub * SUB, sub, partial, bound if sub == count else None, 1)
                    shift, ahead = top(partial), partial
                    for sub in range(subs):
                        ahead = score(half, sub * SUB, at + (count + 1 + sub) * SUB, sub, ahead)
                    run_sum, total = jnp.zeros((8, tile), jnp.float32), None
                    for sub in range(count + 1):
                        probs = weights(sub, shift, 1)
                        run_sum, total = run_sum + jnp.sum(probs, axis=0), value(key + sub * SUB, probs, total)
                    ot_ref[half] = total
                    sum_ref[half] = run_sum
                    used_max_ref[half] = shift
                    max_ref[half] = jnp.where(full_steps > 0, top(ahead), shift)

            def step(index, last):
                key = pl.multiple_of((index - 1) * BIG, BIG)
                at = pl.multiple_of(start + (rest_subs + 1) * SUB + index * BIG, SUB)
                shift = max_ref[half]
                decay = jnp.exp2(used_max_ref[half] - shift)
                run_sum, total, partial = sum_ref[half] * decay, None, lowest
                for sub in range(subs):
                    probs = weights(sub, shift)
                    run_sum = run_sum + jnp.sum(probs, axis=0)
                    if not last:
                        partial = score(half, key + BIG + sub * SUB, at + sub * SUB, sub, partial)
                    total = value(key + sub * SUB, probs, total)
                sum_ref[half] = run_sum
                rescaled(half, total, decay)
                used_max_ref[half] = shift
                if not last:
                    max_ref[half] = jnp.maximum(shift, top(partial))

            def inner_step(index, carry):
                step(index, False)
                return carry

            lax.fori_loop(1, full_steps, inner_step, 0)

            @pl.when(full_steps > 0)
            def _():
                step(full_steps, True)

            return inner

        def turn_inputs(half):
            row = geometry(half)[4]
            qt_ref[half] = q_ref[pl.ds(row, tile), :].T
            gt_ref[half] = g_ref[pl.ds(row, tile), :].T

        def finish_forward(half):
            row = geometry(half)[4]
            row_sum = jnp.sum(sum_ref[half], axis=0, keepdims=True)
            out = (ot_ref[half] / row_sum).astype(jnp.bfloat16)
            o_ref[pl.ds(row, tile), :] = out.T
            max_ref[half] = used_max_ref[half] + wide(jnp.log2(row_sum))
            sum_ref[half] = wide(jnp.sum(out.astype(jnp.float32) * gt_ref[half].astype(jnp.float32), axis=0, keepdims=True))

        def finish_backward(half):
            row = geometry(half)[4]
            dq_ref[pl.ds(row, tile), :] = (dqt_ref[half] * scale).astype(jnp.bfloat16).T

        def grad(half, key, at, size, row):
            log_sum, d_row, total = max_ref[half], sum_ref[half], None
            for sub in range(0, size, SUB):
                span = pl.ds(key + sub, SUB)
                dprobs = _dot(v_ref[span, :], gt_ref[half])
                probs = jnp.exp2(fold(strip[pl.ds(at + sub, SUB), :]) * log2_scale - log_sum[None])
                dscores = probs * (fold(dprobs) - d_row[None])
                probs = probs.reshape(SUB, tile).astype(jnp.bfloat16)
                dscores = dscores.reshape(SUB, tile).astype(jnp.bfloat16)
                dv_ref[span, :] += _dot(probs, g_ref[pl.ds(row, tile), :])
                dk_ref[span, :] += _dot(dscores, q_ref[pl.ds(row, tile), :])
                total = add(total, _dot_first(k_ref[span, :], dscores))
            dqt_ref[half] += total

        def backward_pass(half, inner):
            bound, full_steps, rest_subs, start, row = geometry(half)
            main = start + (rest_subs + 1) * SUB

            def step(index, carry):
                key = pl.multiple_of(index * 2 * BIG, BIG)
                grad(half, key, pl.multiple_of(main + key, SUB), 2 * BIG, row)
                return carry

            lax.fori_loop(0, full_steps // 2, step, 0)

            @pl.when(full_steps % 2 == 1)
            def _():
                key = pl.multiple_of((full_steps - 1) * BIG, BIG)
                grad(half, key, pl.multiple_of(main + key, SUB), BIG, row)

            for count in range(subs):

                @pl.when(rest_subs == count)
                def _():
                    grad(half, pl.multiple_of(full_steps * BIG, BIG), pl.multiple_of(start, SUB), (count + 1) * SUB, row)

            return inner

        between(pair_index, 0)
        for half in range(2):
            turn_inputs(half)
            dqt_ref[half] = jnp.zeros((head_dim, tile), jnp.float32)
        lax.fori_loop(0, 2, forward_pass, 0)
        between(pair_index, 1)
        for half in range(2):
            finish_forward(half)
        lax.fori_loop(0, 2, backward_pass, 0)
        for half in range(2):
            finish_backward(half)
        return carry

    lax.fori_loop(0, half_len // POS, pair, 0)


def _work_shapes(seq_len, head_dim, tile):
    strip_rows = (seq_len // SUB + 3 + BIG // SUB) * SUB
    return [
        pltpu.VMEM((strip_rows, tile), jnp.float32),
        pltpu.VMEM((2, BIG, tile), jnp.float32),
        pltpu.VMEM((2, head_dim, tile), jnp.bfloat16),
        pltpu.VMEM((2, head_dim, tile), jnp.bfloat16),
        pltpu.VMEM((2, head_dim, tile), jnp.float32),
        pltpu.VMEM((2, head_dim, tile), jnp.float32),
        pltpu.VMEM((2, 8, tile), jnp.float32),
        pltpu.VMEM((2, 8, tile), jnp.float32),
        pltpu.VMEM((2, 8, tile), jnp.float32),
    ]


MESH = pl.DeviceIdType.MESH
SLOTS = 6

GATHER_AT = {1: (-1, 1, 3, 4, 5), 2: (0, 2, 5, 6, 9), 3: (1, 5, 8, 10, 15), 4: (11, 14, 16, 19, 22)}


def _gather_at(seq):
    if seq in GATHER_AT:
        return GATHER_AT[seq]
    return tuple(SLOTS * (seq - 2) + gap for gap in (2, 4, 6, 8, 10))


def _kernel(ctx_size, heads, q_hbm, g_hbm, k_hbm, v_hbm, o_hbm, dq_hbm, dk_hbm, dv_hbm, kv_all, *scratch):
    (
        qg_buf,
        od_buf,
        kv_buf,
        acc,
        part,
        ring_in,
        out_buf,
        gather_recv,
        gather_send,
        gather_peer_recv,
        gather_peer_send,
        load_sem,
        qg_sem,
        od_sem,
        peer_recv,
        peer_send,
        ring_recv,
        ring_send,
        out_sem,
        peer_credit,
        side_credit,
        *work,
    ) = scratch
    batch, shard_len, head_dim = k_hbm.shape
    half_len = shard_len // 2
    chips = ctx_size // 2
    last_piece = 2 * ctx_size - 1
    me = lax.axis_index("ctx")
    chip, core = me // 2, me % 2

    def device(which_chip, which_core):
        return lax.rem(which_chip + 2 * chips, chips) * 2 + which_core

    peer = device(chip, 1 - core)
    sides = (device(chip + 1, core), device(chip - 1, core))

    def remote(src, dst, send_sem, recv_sem, target):
        return pltpu.make_async_remote_copy(
            src_ref=src, dst_ref=dst, send_sem=send_sem, recv_sem=recv_sem, device_id={"ctx": target}, device_id_type=MESH
        )

    def wait_recv(ref, sem, target):
        remote(ref, ref, sem, sem, target).wait_recv()

    def wait_send(ref, sem, target):
        remote(ref, ref, sem, sem, target).wait_send()

    def wait_local(ref, sem):
        pltpu.make_async_copy(ref, ref, sem).wait()

    def piece_rows(dev, half):
        piece = dev + half * (last_piece - 2 * dev)
        return pl.ds(pl.multiple_of(piece * half_len, half_len), half_len)

    def shard_refs(seq, dev, which):
        if seq == 0:
            return [kv_buf.at[0, which, piece_rows(dev, half), :] for half in range(2)]
        return [kv_all.at[seq, 2 * dev + which]]

    def send_shard(sources, seq, dev, which, targets):
        for target, send_sem, recv_sem in targets:
            for source, place in zip(sources, shard_refs(seq, dev, which)):
                remote(source, place, send_sem, recv_sem, target).start()

    def to_side(way, seq, which, hop):
        return sides[way], gather_send.at[way, seq], gather_recv.at[way, which, seq, hop]

    def to_peer(seq):
        return peer, gather_peer_send.at[seq], gather_peer_recv.at[seq]

    def gather_send_own(seq):
        for which, source in enumerate((k_hbm, v_hbm)):
            sources = [source.at[seq]]
            if seq == 0:
                sources = [source.at[seq, pl.ds(half * half_len, half_len), :] for half in range(2)]
            send_shard(sources, seq, me, which, [to_side(0, seq, which, 0), to_side(1, seq, which, 0), to_peer(seq)])

    def gather_arrival(seq, hop):
        for which in range(2):
            for way in range(2) if hop < 4 else (which,):
                origin = device(chip - hop if way == 0 else chip + hop, core)
                refs = shard_refs(seq, origin, which)
                wait_recv(kv_all.at[0, 0], gather_recv.at[way, which, seq, hop - 1], sides[way])
                onward = [to_side(way, seq, which, hop)] if hop < (4 if way == which else 3) else []
                send_shard(refs, seq, origin, which, onward + [to_peer(seq)])

    def drain(seq, carry):
        for way in range(2):
            wait_send(kv_all.at[0, pl.ds(0, 7)], gather_send.at[way, seq], sides[way])
        wait_send(kv_all.at[0, pl.ds(0, ctx_size)], gather_peer_send.at[seq], peer)
        return carry

    def load_keys(seq):
        wait_recv(kv_all.at[seq, pl.ds(0, ctx_size)], gather_peer_recv.at[seq], peer)
        slot = seq % 2

        def each(dev, carry):
            for half in range(2):
                piece = dev + half * (last_piece - 2 * dev)
                there = pl.ds(half * half_len, half_len)
                here = pl.ds(pl.multiple_of(piece * half_len, half_len), half_len)
                for which, own in enumerate((k_hbm, v_hbm)):
                    target = kv_buf.at[slot, which, here, :]

                    @pl.when(dev == me)
                    def _():
                        pltpu.make_async_copy(own.at[seq, there, :], target, load_sem.at[slot]).start()

                    @pl.when(dev != me)
                    def _():
                        pltpu.make_async_copy(kv_all.at[seq, 2 * dev + which, there, :], target, load_sem.at[slot]).start()

            return carry

        lax.fori_loop(0, ctx_size, each, 0)

    chunk_order = (chips // 2, chips // 2 - 1, chips // 2 + 1, chips // 2 - 2, chips // 2 + 2, 1, chips - 1, 0)

    def chunk_chip(offset):
        return lax.rem(chip + offset, chips)

    def reduce_peer_send(seq):
        slot = seq % 2

        @pl.when(seq >= 2)
        def _():
            pl.semaphore_wait(peer_credit, 1)

        for index, offset in enumerate(chunk_order):
            where = chunk_chip(offset)
            for half in range(2):
                for which in range(2):
                    remote(
                        acc.at[which, piece_rows(2 * where + 1 - core, half), :],
                        part.at[slot, 2 * where + which, pl.ds(half * half_len, half_len), :],
                        peer_send.at[slot],
                        peer_recv.at[slot, index],
                        peer,
                    ).start()

    def clear_grads():
        def each(step, carry):
            for which in range(2):
                acc[which, pl.ds(pl.multiple_of(step * SUB, SUB), SUB), :] = jnp.zeros((SUB, head_dim), jnp.float32)
            return carry

        lax.fori_loop(0, acc.shape[1] // SUB, each, 0)

    def ring_chunk(slot, step, way, which):
        return part.at[slot, 2 * chunk_chip(5 - step if way == 0 else chips - 5 + step) + which]

    def ring_send_step(slot, step, way, which):
        remote(
            ring_chunk(slot, step, way, which),
            ring_in.at[slot, way, which, step - 1],
            ring_send.at[slot, way],
            ring_recv.at[slot, way, which, step - 1],
            sides[way],
        ).start()

    def ring_wait(slot, step, way, which):
        wait_recv(ring_in.at[slot, way, which, step - 1], ring_recv.at[slot, way, which, step - 1], sides[way])

    def reduce_begin(seq):
        slot = seq % 2

        @pl.when(seq >= 2)
        def _():
            for way in range(2):
                pl.semaphore_wait(side_credit.at[way], 1)

        for index, offset in enumerate(chunk_order):
            where = chunk_chip(offset)
            wait_recv(part.at[slot, pl.ds(2 * where, 2)], peer_recv.at[slot, index], peer)
            for half in range(2):
                for which in range(2):
                    place = pl.ds(half * half_len, half_len)
                    part[slot, 2 * where + which, place, :] += acc[which, piece_rows(2 * where + core, half), :]
            if index == 0:
                for way in range(2):
                    ring_send_step(slot, 1, way, way)
            elif index < 3:
                ring_send_step(slot, 2, index - 1, 2 - index)
        wait_send(part.at[slot], peer_send.at[slot], peer)
        clear_grads()

    def reduce_step(seq, step, long_chain):
        slot = seq % 2
        for way in range(2):
            which = way if long_chain else 1 - way
            ring_wait(slot, step - 1, way, which)
            ring_chunk(slot, step, way, which)[...] += ring_in[slot, way, which, step - 2]
        for way in range(2):
            ring_send_step(slot, step, way, way if long_chain else 1 - way)

    def reduce_end(seq):
        slot = seq % 2

        @pl.when(seq >= 2)
        def _():
            wait_local(out_buf.at[slot], out_sem.at[slot])

        for which, target in enumerate((dk_hbm, dv_hbm)):
            for way in (1 - which, which):
                ring_wait(slot, 4, way, which)
            total = part[slot, 2 * chip + which] + ring_in[slot, 0, which, 3] + ring_in[slot, 1, which, 3]
            out_buf[slot, which] = (total * (head_dim**-0.5) if which == 0 else total).astype(jnp.bfloat16)
            pltpu.make_async_copy(out_buf.at[slot, which], target.at[seq], out_sem.at[slot]).start()
        for way in range(2):
            wait_send(part.at[slot, pl.ds(0, 7)], ring_send.at[slot, way], sides[way])

        @pl.when(seq + 2 < batch)
        def _():
            pl.semaphore_signal(peer_credit, 1, device_id={"ctx": peer}, device_id_type=MESH)
            for way in range(2):
                pl.semaphore_signal(side_credit.at[1 - way], 1, device_id={"ctx": sides[way]}, device_id_type=MESH)

    def load_rows(seq):
        for which, source in enumerate((q_hbm, g_hbm)):
            pltpu.make_async_copy(source.at[seq], qg_buf.at[seq % 2, which], qg_sem.at[seq % 2]).start()

    load_rows(0)
    clear_grads()
    barrier = pltpu.get_barrier_semaphore()
    for target in (*sides, peer):
        pl.semaphore_signal(barrier, 1, device_id={"ctx": target}, device_id_type=MESH)
    pl.semaphore_wait(barrier, 3)

    gather_send_own(0)
    own_loads = [
        pltpu.make_async_copy(source.at[0, pl.ds(half * half_len, half_len), :], place, load_sem.at[0])
        for which, source in enumerate((k_hbm, v_hbm))
        for half, place in enumerate(shard_refs(0, me, which))
    ]
    for copy in own_loads:
        copy.start()
    for hop in range(1, 4):
        gather_arrival(0, hop)
    gather_send_own(1)
    gather_arrival(0, 4)
    wait_recv(kv_all.at[0, pl.ds(0, ctx_size)], gather_peer_recv.at[0], peer)
    wait_local(kv_all.at[0, pl.ds(0, 2)], load_sem.at[0])

    events = [[] for _ in range(SLOTS)]
    for seq in range(1, batch):
        for hop, at in enumerate(_gather_at(seq)):
            if at >= 0:
                event = functools.partial(gather_arrival, seq, hop) if hop else functools.partial(gather_send_own, seq)
                events[at % SLOTS].append((at // SLOTS, event))

    events[0].append((1, functools.partial(drain, 0, 0)))

    def steps(*which):
        return lambda seq: [reduce_step(seq, *one) for one in which]

    last = batch - 1
    reduce_events = {
        (0, 1): reduce_peer_send,
        (1, 1): reduce_begin,
        (2, 1): steps((2, True)),
        (3, 1): steps((3, False)),
        (4, 1): steps((3, True)),
        (5, 1): steps((4, False)),
        (0, 2): steps((4, True)),
        (3, 2): reduce_end,
    }
    last_events = {
        (0, 1): reduce_peer_send,
        (1, 1): reduce_begin,
        (2, 1): steps((2, True)),
        (3, 1): steps((3, False), (3, True)),
        (5, 1): steps((4, False), (4, True)),
        (0, 2): reduce_events[0, 2],
        (3, 2): reduce_end,
    }

    def sequence(seq, carry):
        slot = seq % 2

        @pl.when(seq >= 1)
        def _():
            wait_local(kv_buf.at[slot], load_sem.at[slot])

        wait_local(qg_buf.at[slot], qg_sem.at[slot])

        @pl.when(seq >= 2)
        def _():
            wait_local(od_buf.at[slot], od_sem.at[slot])

        @pl.when(seq + 1 < batch)
        def _():
            load_rows(seq + 1)

        def between(pair_index, pass_index):
            for pair in range(SLOTS // 2):
                at = 2 * pair + pass_index

                @pl.when(pair_index == pair)
                def _():
                    for when, event in events[at]:

                        @pl.when(seq == when)
                        def _():
                            event()

                    for lag in (2, 1):
                        usual, final = reduce_events.get((at, lag)), last_events.get((at, lag))
                        if usual and usual is final:

                            @pl.when(seq >= lag)
                            def _():
                                usual(seq - lag)

                        elif usual or final:

                            @pl.when((seq >= lag) & (seq < last))
                            def _():
                                if usual:
                                    usual(seq - lag)

                            @pl.when(seq == last)
                            def _():
                                if final:
                                    final(seq - lag)

                    if at == SLOTS - 1:

                        @pl.when(seq + 1 < batch)
                        def _():
                            load_keys(seq + 1)

        _attention_sequence(
            me,
            ctx_size,
            heads,
            qg_buf.at[slot, 0],
            qg_buf.at[slot, 1],
            kv_buf.at[slot, 0],
            kv_buf.at[slot, 1],
            od_buf.at[slot, 0],
            od_buf.at[slot, 1],
            acc.at[0],
            acc.at[1],
            work,
            between,
        )
        for which, target in enumerate((o_hbm, dq_hbm)):
            pltpu.make_async_copy(od_buf.at[slot, which], target.at[seq], od_sem.at[slot]).start()
        return carry

    lax.fori_loop(0, batch, sequence, 0)

    reduce_peer_send(last)
    reduce_begin(last)
    reduce_step(last, 2, True)
    reduce_end(last - 1)
    for step in range(3, 5):
        reduce_step(last, step, False)
        reduce_step(last, step, True)
    reduce_end(last)
    for slot in range(2):
        wait_local(od_buf.at[slot], od_sem.at[slot])
        wait_local(out_buf.at[slot], out_sem.at[slot])

    lax.fori_loop(1, batch, drain, 0)


def solution(mesh):
    ctx_size = mesh.shape["ctx"]
    block_spec = P("data", "ctx", None, None)

    def local_attention(queries, keys_in, values_in, grad_out):
        batch, shard_len, heads, head_dim = queries.shape
        rows, seq_len, tile = shard_len * heads, shard_len * ctx_size, POS * heads
        row_shape = jax.ShapeDtypeStruct((batch, rows, head_dim), jnp.bfloat16)
        shard_shape = jax.ShapeDtypeStruct((batch, shard_len, head_dim), jnp.bfloat16)
        dma, regular = pltpu.SemaphoreType.DMA, pltpu.SemaphoreType.REGULAR
        attn_out, grad_q, grad_k, grad_v, _ = pl.pallas_call(
            functools.partial(_kernel, ctx_size, heads),
            out_shape=[
                row_shape,
                row_shape,
                shard_shape,
                shard_shape,
                jax.ShapeDtypeStruct((batch, 2 * ctx_size, shard_len, head_dim), jnp.bfloat16),
            ],
            in_specs=[pl.BlockSpec(memory_space=pl.ANY)] * 4,
            out_specs=[pl.BlockSpec(memory_space=pl.ANY)] * 5,
            scratch_shapes=[
                pltpu.VMEM((2, 2, rows, head_dim), jnp.bfloat16),
                pltpu.VMEM((2, 2, rows, head_dim), jnp.bfloat16),
                pltpu.VMEM((2, 2, seq_len, head_dim), jnp.bfloat16),
                pltpu.VMEM((2, seq_len, head_dim), jnp.float32),
                pltpu.VMEM((2, ctx_size, shard_len, head_dim), jnp.float32),
                pltpu.VMEM((2, 2, 2, 4, shard_len, head_dim), jnp.float32),
                pltpu.VMEM((2, 2, shard_len, head_dim), jnp.bfloat16),
                dma((2, 2, batch, 4)),
                dma((2, batch)),
                dma((batch,)),
                dma((batch,)),
                dma((2,)),
                dma((2,)),
                dma((2,)),
                dma((2, ctx_size // 2)),
                dma((2,)),
                dma((2, 2, 2, 4)),
                dma((2, 2)),
                dma((2,)),
                regular,
                regular((2,)),
            ]
            + _work_shapes(seq_len, head_dim, tile),
            compiler_params=pltpu.CompilerParams(vmem_limit_bytes=VMEM_BYTES, collective_id=0, has_side_effects=True),
            cost_estimate=pl.CostEstimate(flops=10**11, bytes_accessed=10**8, transcendentals=0),
        )(
            queries.reshape(batch, rows, head_dim),
            grad_out.reshape(batch, rows, head_dim),
            keys_in.reshape(batch, shard_len, head_dim),
            values_in.reshape(batch, shard_len, head_dim),
        )
        return attn_out.reshape(queries.shape), grad_q.reshape(queries.shape), grad_k.reshape(keys_in.shape), grad_v.reshape(values_in.shape)

    return jax.shard_map(local_attention, mesh=mesh, in_specs=(block_spec,) * 4, out_specs=(block_spec,) * 4, check_vma=False)
```

```python
import functools
import math

import jax
import jax.numpy as jnp
from jax import lax
from jax.experimental import pallas as pl
from jax.experimental.pallas import tpu as pltpu
from jax.sharding import PartitionSpec as P

MASK_VALUE = -1e30
BIG = 1024
SUB = 256
POS = 64
VMEM_BYTES = 60 * 2**20


def _dot_first(lhs, rhs):
    return lax.dot_general(lhs, rhs, (((0,), (0,)), ((), ())), preferred_element_type=jnp.float32)


def _dot(lhs, rhs):
    return lax.dot_general(lhs, rhs, (((1,), (0,)), ((), ())), preferred_element_type=jnp.float32)


def _attention_sequence(my_index, ctx_size, heads, q_ref, g_ref, k_ref, v_ref, o_ref, dq_ref, dk_ref, dv_ref, work, between):
    strip, recent, qt_ref, gt_ref, ot_ref, dqt_ref, max_ref, used_max_ref, sum_ref = work
    head_dim = k_ref.shape[1]
    rows = q_ref.shape[0]
    half_len = rows // heads // 2
    tile = POS * heads
    subs = BIG // SUB
    scale = head_dim**-0.5
    log2_scale = scale * math.log2(math.e)
    last_piece = 2 * ctx_size - 1

    lowest = jnp.full((8, tile), MASK_VALUE, jnp.float32)

    def wide(row):
        return jnp.broadcast_to(row, (8, tile))

    def top(partial):
        return wide(jnp.max(partial, axis=0, keepdims=True)) * log2_scale

    def fold(block):
        return block.reshape(block.shape[0] // 8, 8, tile)

    def add(total, part):
        return part if total is None else total + part

    def pair(pair_index, carry):
        low_subs = (my_index * half_len + POS * (pair_index + 1) - 1) // SUB + 1

        def geometry(half):
            piece = my_index + half * (last_piece - 2 * my_index)
            bound = piece * half_len + POS * (pair_index + 1)
            full_subs = (bound - 1) // SUB
            row = pl.multiple_of(half * (rows // 2) + pair_index * tile, tile)
            return bound, full_subs // subs, full_subs % subs, half * low_subs * SUB, row

        def score(half, key, at, sub, partial, bound=None, into=0):
            scores = _dot(k_ref[pl.ds(key, SUB), :], qt_ref[half])
            if bound is not None:
                key_pos = key + lax.broadcasted_iota(jnp.int32, (SUB, 1), 0)
                query_pos = bound - POS + lax.broadcasted_iota(jnp.int32, (1, tile), 1) // heads
                scores = jnp.where(key_pos <= query_pos, scores, MASK_VALUE)
            strip[pl.ds(at, SUB), :] = scores
            recent[into, sub * SUB : (sub + 1) * SUB, :] = scores
            return jnp.maximum(partial, jnp.max(fold(scores), axis=0))

        def weights(sub, shift, source=0):
            return jnp.exp2(fold(recent[source, sub * SUB : (sub + 1) * SUB, :]) * log2_scale - shift[None])

        def value(key, probs, total):
            return add(total, _dot_first(v_ref[pl.ds(key, SUB), :], probs.reshape(SUB, tile).astype(jnp.bfloat16)))

        def rescaled(half, total, decay):
            ot_ref[half] = (fold(ot_ref[half]) * decay[None]).reshape(head_dim, tile) + total

        def value_step(half, index, row_scores):
            key = pl.multiple_of((index - 1) * BIG, BIG)
            shift = max_ref[half]
            decay = jnp.exp2(used_max_ref[half] - shift)
            run_sum, total = sum_ref[half] * decay, None
            for sub in range(subs):
                probs = weights(sub, shift)
                run_sum = run_sum + jnp.sum(probs, axis=0)
                row_scores(sub)
                total = value(key + sub * SUB, probs, total)
            sum_ref[half] = run_sum
            rescaled(half, total, decay)
            used_max_ref[half] = shift

        def forward_start(half, behind):
            bound, full_steps, rest_subs, start, row = geometry(half)
            for count in range(subs):
                for flag in (False, True):
                    is_behind, has_main = (flag, True) if half else (False, flag)

                    @pl.when((rest_subs == count) & (((behind if half else full_steps) > 0) == flag))
                    def _():
                        key, at = pl.multiple_of(full_steps * BIG, BIG), pl.multiple_of(start, SUB)
                        partial = lowest
                        for sub in range(count + 1):
                            last_keys = bound if sub == count else None
                            partial = score(half, key + sub * SUB, at + sub * SUB, sub, partial, last_keys, 1)
                        ahead = [partial]

                        def first_block(sub):
                            ahead[0] = score(half, sub * SUB, at + (count + 1 + sub) * SUB, sub, ahead[0])

                        if is_behind:
                            value_step(1 - half, behind, first_block)
                        elif has_main:
                            for sub in range(subs):
                                first_block(sub)
                        shift = top(partial)
                        run_sum, total = jnp.zeros((8, tile), jnp.float32), None
                        for sub in range(count + 1):
                            probs = weights(sub, shift, 1)
                            run_sum, total = run_sum + jnp.sum(probs, axis=0), value(key + sub * SUB, probs, total)
                        ot_ref[half] = total
                        sum_ref[half] = run_sum
                        used_max_ref[half] = shift
                        max_ref[half] = top(ahead[0]) if has_main else shift

        def forward_rest(half):
            _, full_steps, rest_subs, start, _ = geometry(half)

            def step(index, carry):
                at = pl.multiple_of(start + (rest_subs + 1) * SUB + index * BIG, SUB)
                partial = [lowest]

                def next_block(sub):
                    partial[0] = score(half, pl.multiple_of(index * BIG, BIG) + sub * SUB, at + sub * SUB, sub, partial[0])

                shift = max_ref[half]
                value_step(half, index, next_block)
                max_ref[half] = jnp.maximum(shift, top(partial[0]))
                return carry

            lax.fori_loop(1, full_steps, step, 0)

        def turn_inputs(half):
            row = geometry(half)[4]
            qt_ref[half] = q_ref[pl.ds(row, tile), :].T
            gt_ref[half] = g_ref[pl.ds(row, tile), :].T

        def finish_forward(half):
            row = geometry(half)[4]
            row_sum = jnp.sum(sum_ref[half], axis=0, keepdims=True)
            out = (ot_ref[half] / row_sum).astype(jnp.bfloat16)
            o_ref[pl.ds(row, tile), :] = out.T
            max_ref[half] = used_max_ref[half] + wide(jnp.log2(row_sum))
            sum_ref[half] = wide(jnp.sum(out.astype(jnp.float32) * gt_ref[half].astype(jnp.float32), axis=0, keepdims=True))

        def finish_backward(half):
            row = geometry(half)[4]
            dq_ref[pl.ds(row, tile), :] = (dqt_ref[half] * scale).astype(jnp.bfloat16).T

        def grad(half, key, at, size, row):
            log_sum, d_row, total = max_ref[half], sum_ref[half], None
            for sub in range(0, size, SUB):
                span = pl.ds(key + sub, SUB)
                dprobs = _dot(v_ref[span, :], gt_ref[half])
                probs = jnp.exp2(fold(strip[pl.ds(at + sub, SUB), :]) * log2_scale - log_sum[None])
                dscores = probs * (fold(dprobs) - d_row[None])
                probs = probs.reshape(SUB, tile).astype(jnp.bfloat16)
                dscores = dscores.reshape(SUB, tile).astype(jnp.bfloat16)
                dv_ref[span, :] += _dot(probs, g_ref[pl.ds(row, tile), :])
                dk_ref[span, :] += _dot(dscores, q_ref[pl.ds(row, tile), :])
                total = add(total, _dot_first(k_ref[span, :], dscores))
            dqt_ref[half] += total

        def backward_pass(half, inner):
            bound, full_steps, rest_subs, start, row = geometry(half)
            main = start + (rest_subs + 1) * SUB

            def step(index, carry):
                key = pl.multiple_of(index * 2 * BIG, BIG)
                grad(half, key, pl.multiple_of(main + key, SUB), 2 * BIG, row)
                return carry

            lax.fori_loop(0, full_steps // 2, step, 0)

            @pl.when(full_steps % 2 == 1)
            def _():
                key = pl.multiple_of((full_steps - 1) * BIG, BIG)
                grad(half, key, pl.multiple_of(main + key, SUB), BIG, row)

            for count in range(subs):

                @pl.when(rest_subs == count)
                def _():
                    grad(half, pl.multiple_of(full_steps * BIG, BIG), pl.multiple_of(start, SUB), (count + 1) * SUB, row)

            return inner

        between(pair_index, 0)
        for half in range(2):
            turn_inputs(half)
            dqt_ref[half] = jnp.zeros((head_dim, tile), jnp.float32)
        low_steps, high_steps = geometry(0)[1], geometry(1)[1]
        forward_start(0, None)
        forward_rest(0)
        forward_start(1, low_steps)
        forward_rest(1)
        value_step(1, high_steps, lambda sub: None)
        between(pair_index, 1)
        for half in range(2):
            finish_forward(half)
        lax.fori_loop(0, 2, backward_pass, 0)
        for half in range(2):
            finish_backward(half)
        return carry

    lax.fori_loop(0, half_len // POS, pair, 0)


def _work_shapes(seq_len, head_dim, tile):
    strip_rows = (seq_len // SUB + 3 + BIG // SUB) * SUB
    return [
        pltpu.VMEM((strip_rows, tile), jnp.float32),
        pltpu.VMEM((2, BIG, tile), jnp.float32),
        pltpu.VMEM((2, head_dim, tile), jnp.bfloat16),
        pltpu.VMEM((2, head_dim, tile), jnp.bfloat16),
        pltpu.VMEM((2, head_dim, tile), jnp.float32),
        pltpu.VMEM((2, head_dim, tile), jnp.float32),
        pltpu.VMEM((2, 8, tile), jnp.float32),
        pltpu.VMEM((2, 8, tile), jnp.float32),
        pltpu.VMEM((2, 8, tile), jnp.float32),
    ]


MESH = pl.DeviceIdType.MESH
SLOTS = 6

GATHER_AT = {1: (-1, 1, 3, 4, 5), 2: (0, 2, 5, 6, 9), 3: (1, 5, 8, 10, 15), 4: (11, 14, 16, 19, 22)}


def _gather_at(seq):
    if seq in GATHER_AT:
        return GATHER_AT[seq]
    return tuple(SLOTS * (seq - 2) + gap for gap in (2, 4, 6, 8, 10))


def _kernel(ctx_size, heads, q_hbm, g_hbm, k_hbm, v_hbm, o_hbm, dq_hbm, dk_hbm, dv_hbm, kv_all, *scratch):
    (
        qg_buf,
        od_buf,
        kv_buf,
        acc,
        part,
        ring_in,
        out_buf,
        first_recv,
        gather_recv,
        gather_send,
        gather_peer_recv,
        gather_peer_send,
        load_sem,
        qg_sem,
        od_sem,
        peer_recv,
        peer_send,
        ring_recv,
        ring_send,
        out_sem,
        peer_credit,
        side_credit,
        *work,
    ) = scratch
    batch, shard_len, head_dim = k_hbm.shape
    half_len = shard_len // 2
    chips = ctx_size // 2
    last_piece = 2 * ctx_size - 1
    me = lax.axis_index("ctx")
    chip, core = me // 2, me % 2

    def device(which_chip, which_core):
        return lax.rem(which_chip + 2 * chips, chips) * 2 + which_core

    peer = device(chip, 1 - core)
    sides = (device(chip + 1, core), device(chip - 1, core))

    def remote(src, dst, send_sem, recv_sem, target):
        return pltpu.make_async_remote_copy(
            src_ref=src, dst_ref=dst, send_sem=send_sem, recv_sem=recv_sem, device_id={"ctx": target}, device_id_type=MESH
        )

    def wait_recv(ref, sem, target):
        remote(ref, ref, sem, sem, target).wait_recv()

    def wait_send(ref, sem, target):
        remote(ref, ref, sem, sem, target).wait_send()

    def wait_local(ref, sem):
        pltpu.make_async_copy(ref, ref, sem).wait()

    def piece_rows(dev, half):
        piece = dev + half * (last_piece - 2 * dev)
        return pl.ds(pl.multiple_of(piece * half_len, half_len), half_len)

    def shard_refs(seq, dev, which):
        if seq == 0:
            return [kv_buf.at[0, which, piece_rows(dev, half), :] for half in range(2)]
        return [kv_all.at[seq, 2 * dev + which]]

    def arrived(way, seq, which, hop, part_index):
        return first_recv.at[way, which, part_index, hop] if seq == 0 else gather_recv.at[way, which, seq, hop]

    def send_part(source, place, seq, which, part_index, hops):
        remote(source, place, gather_peer_send.at[seq], gather_peer_recv.at[seq], peer).start()
        for way, hop in hops:
            remote(source, place, gather_send.at[way, seq], arrived(way, seq, which, hop, part_index), sides[way]).start()

    def gather_send_own(seq):
        for which, source in enumerate((k_hbm, v_hbm)):
            sources = [source.at[seq]]
            if seq == 0:
                sources = [source.at[seq, pl.ds(half * half_len, half_len), :] for half in range(2)]
            for part_index, place in enumerate(shard_refs(seq, me, which)):
                send_part(sources[part_index], place, seq, which, part_index, [(0, 0), (1, 0)])

    def gather_arrival(seq, hop):
        for which in range(2):
            for part_index in range(2 if seq == 0 else 1):
                for way in range(2) if hop < 4 else (which,):
                    origin = device(chip - hop if way == 0 else chip + hop, core)
                    place = shard_refs(seq, origin, which)[part_index]
                    wait_recv(place, arrived(way, seq, which, hop - 1, part_index), sides[way])
                    onward = [(way, hop)] if hop < (4 if way == which else 3) else []
                    send_part(place, place, seq, which, part_index, onward)

    def drain(seq, carry):
        for way in range(2):
            wait_send(kv_all.at[0, pl.ds(0, 7)], gather_send.at[way, seq], sides[way])
        wait_send(kv_all.at[0, pl.ds(0, ctx_size)], gather_peer_send.at[seq], peer)
        return carry

    def load_keys(seq):
        wait_recv(kv_all.at[seq, pl.ds(0, ctx_size)], gather_peer_recv.at[seq], peer)
        slot = seq % 2

        def each(dev, carry):
            for half in range(2):
                piece = dev + half * (last_piece - 2 * dev)
                there = pl.ds(half * half_len, half_len)
                here = pl.ds(pl.multiple_of(piece * half_len, half_len), half_len)
                for which, own in enumerate((k_hbm, v_hbm)):
                    target = kv_buf.at[slot, which, here, :]

                    @pl.when(dev == me)
                    def _():
                        pltpu.make_async_copy(own.at[seq, there, :], target, load_sem.at[slot]).start()

                    @pl.when(dev != me)
                    def _():
                        pltpu.make_async_copy(kv_all.at[seq, 2 * dev + which, there, :], target, load_sem.at[slot]).start()

            return carry

        lax.fori_loop(0, ctx_size, each, 0)

    chunk_order = (chips // 2, chips // 2 - 1, chips // 2 + 1, chips // 2 - 2, chips // 2 + 2, 1, chips - 1, 0)

    def chunk_chip(offset):
        return lax.rem(chip + offset, chips)

    def reduce_peer_send(seq):
        slot = seq % 2

        @pl.when(seq >= 2)
        def _():
            pl.semaphore_wait(peer_credit, 1)

        for index, offset in enumerate(chunk_order):
            where = chunk_chip(offset)
            for half in range(2):
                for which in range(2):
                    remote(
                        acc.at[which, piece_rows(2 * where + 1 - core, half), :],
                        part.at[slot, 2 * where + which, pl.ds(half * half_len, half_len), :],
                        peer_send.at[slot],
                        peer_recv.at[slot, index],
                        peer,
                    ).start()

    def clear_grads():
        def each(step, carry):
            for which in range(2):
                acc[which, pl.ds(pl.multiple_of(step * SUB, SUB), SUB), :] = jnp.zeros((SUB, head_dim), jnp.float32)
            return carry

        lax.fori_loop(0, acc.shape[1] // SUB, each, 0)

    def ring_chunk(slot, step, way, which):
        return part.at[slot, 2 * chunk_chip(5 - step if way == 0 else chips - 5 + step) + which]

    def ring_send_step(slot, step, way, which):
        remote(
            ring_chunk(slot, step, way, which),
            ring_in.at[slot, way, which, step - 1],
            ring_send.at[slot, way],
            ring_recv.at[slot, way, which, step - 1],
            sides[way],
        ).start()

    def ring_wait(slot, step, way, which):
        wait_recv(ring_in.at[slot, way, which, step - 1], ring_recv.at[slot, way, which, step - 1], sides[way])

    def reduce_begin(seq):
        slot = seq % 2

        @pl.when(seq >= 2)
        def _():
            for way in range(2):
                pl.semaphore_wait(side_credit.at[way], 1)

        for index, offset in enumerate(chunk_order):
            where = chunk_chip(offset)
            wait_recv(part.at[slot, pl.ds(2 * where, 2)], peer_recv.at[slot, index], peer)
            for half in range(2):
                for which in range(2):
                    place = pl.ds(half * half_len, half_len)
                    part[slot, 2 * where + which, place, :] += acc[which, piece_rows(2 * where + core, half), :]
            if index == 0:
                for way in range(2):
                    ring_send_step(slot, 1, way, way)
            elif index < 3:
                ring_send_step(slot, 2, index - 1, 2 - index)
        wait_send(part.at[slot], peer_send.at[slot], peer)
        clear_grads()

    def reduce_step(seq, step, long_chain):
        slot = seq % 2
        for way in range(2):
            which = way if long_chain else 1 - way
            ring_wait(slot, step - 1, way, which)
            ring_chunk(slot, step, way, which)[...] += ring_in[slot, way, which, step - 2]
        for way in range(2):
            ring_send_step(slot, step, way, way if long_chain else 1 - way)

    def reduce_end(seq):
        slot = seq % 2

        @pl.when(seq >= 2)
        def _():
            wait_local(out_buf.at[slot], out_sem.at[slot])

        for which, target in enumerate((dk_hbm, dv_hbm)):
            for way in (1 - which, which):
                ring_wait(slot, 4, way, which)
            total = part[slot, 2 * chip + which] + ring_in[slot, 0, which, 3] + ring_in[slot, 1, which, 3]
            out_buf[slot, which] = (total * (head_dim**-0.5) if which == 0 else total).astype(jnp.bfloat16)
            pltpu.make_async_copy(out_buf.at[slot, which], target.at[seq], out_sem.at[slot]).start()
        for way in range(2):
            wait_send(part.at[slot, pl.ds(0, 7)], ring_send.at[slot, way], sides[way])

        @pl.when(seq + 2 < batch)
        def _():
            pl.semaphore_signal(peer_credit, 1, device_id={"ctx": peer}, device_id_type=MESH)
            for way in range(2):
                pl.semaphore_signal(side_credit.at[1 - way], 1, device_id={"ctx": sides[way]}, device_id_type=MESH)

    def load_rows(seq):
        for which, source in enumerate((q_hbm, g_hbm)):
            pltpu.make_async_copy(source.at[seq], qg_buf.at[seq % 2, which], qg_sem.at[seq % 2]).start()

    load_rows(0)
    clear_grads()
    barrier = pltpu.get_barrier_semaphore()
    for target in (*sides, peer):
        pl.semaphore_signal(barrier, 1, device_id={"ctx": target}, device_id_type=MESH)
    pl.semaphore_wait(barrier, 3)

    gather_send_own(0)
    own_loads = [
        pltpu.make_async_copy(source.at[0, pl.ds(half * half_len, half_len), :], place, load_sem.at[0])
        for which, source in enumerate((k_hbm, v_hbm))
        for half, place in enumerate(shard_refs(0, me, which))
    ]
    for copy in own_loads:
        copy.start()
    for hop in range(1, 4):
        gather_arrival(0, hop)
    gather_send_own(1)
    gather_arrival(0, 4)
    wait_recv(kv_all.at[0, pl.ds(0, ctx_size)], gather_peer_recv.at[0], peer)
    wait_local(kv_all.at[0, pl.ds(0, 2)], load_sem.at[0])

    events = [[] for _ in range(SLOTS)]
    for seq in range(1, batch):
        for hop, at in enumerate(_gather_at(seq)):
            if at >= 0:
                event = functools.partial(gather_arrival, seq, hop) if hop else functools.partial(gather_send_own, seq)
                events[at % SLOTS].append((at // SLOTS, event))

    events[0].append((1, functools.partial(drain, 0, 0)))

    def steps(*which):
        return lambda seq: [reduce_step(seq, *one) for one in which]

    last = batch - 1
    reduce_events = {
        (0, 1): reduce_peer_send,
        (1, 1): reduce_begin,
        (2, 1): steps((2, True)),
        (3, 1): steps((3, False)),
        (4, 1): steps((3, True)),
        (5, 1): steps((4, False)),
        (0, 2): steps((4, True)),
        (3, 2): reduce_end,
    }
    last_events = {
        (0, 1): reduce_peer_send,
        (1, 1): reduce_begin,
        (2, 1): steps((2, True)),
        (3, 1): steps((3, False), (3, True)),
        (5, 1): steps((4, False), (4, True)),
        (0, 2): reduce_events[0, 2],
        (3, 2): reduce_end,
    }

    def sequence(seq, carry):
        slot = seq % 2

        @pl.when(seq >= 1)
        def _():
            wait_local(kv_buf.at[slot], load_sem.at[slot])

        wait_local(qg_buf.at[slot], qg_sem.at[slot])

        @pl.when(seq >= 2)
        def _():
            wait_local(od_buf.at[slot], od_sem.at[slot])

        @pl.when(seq + 1 < batch)
        def _():
            load_rows(seq + 1)

        def between(pair_index, pass_index):
            for pair in range(SLOTS // 2):
                at = 2 * pair + pass_index

                @pl.when(pair_index == pair)
                def _():
                    for when, event in events[at]:

                        @pl.when(seq == when)
                        def _():
                            event()

                    for lag in (2, 1):
                        usual, final = reduce_events.get((at, lag)), last_events.get((at, lag))
                        if usual and usual is final:

                            @pl.when(seq >= lag)
                            def _():
                                usual(seq - lag)

                        elif usual or final:

                            @pl.when((seq >= lag) & (seq < last))
                            def _():
                                if usual:
                                    usual(seq - lag)

                            @pl.when(seq == last)
                            def _():
                                if final:
                                    final(seq - lag)

                    if at == SLOTS - 1:

                        @pl.when(seq + 1 < batch)
                        def _():
                            load_keys(seq + 1)

        _attention_sequence(
            me,
            ctx_size,
            heads,
            qg_buf.at[slot, 0],
            qg_buf.at[slot, 1],
            kv_buf.at[slot, 0],
            kv_buf.at[slot, 1],
            od_buf.at[slot, 0],
            od_buf.at[slot, 1],
            acc.at[0],
            acc.at[1],
            work,
            between,
        )
        for which, target in enumerate((o_hbm, dq_hbm)):
            pltpu.make_async_copy(od_buf.at[slot, which], target.at[seq], od_sem.at[slot]).start()
        return carry

    lax.fori_loop(0, batch, sequence, 0)

    reduce_peer_send(last)
    reduce_begin(last)
    reduce_step(last, 2, True)
    reduce_end(last - 1)
    for step in range(3, 5):
        reduce_step(last, step, False)
        reduce_step(last, step, True)
    reduce_end(last)
    for slot in range(2):
        wait_local(od_buf.at[slot], od_sem.at[slot])
        wait_local(out_buf.at[slot], out_sem.at[slot])

    lax.fori_loop(1, batch, drain, 0)


def solution(mesh):
    ctx_size = mesh.shape["ctx"]
    block_spec = P("data", "ctx", None, None)

    def local_attention(queries, keys_in, values_in, grad_out):
        batch, shard_len, heads, head_dim = queries.shape
        rows, seq_len, tile = shard_len * heads, shard_len * ctx_size, POS * heads
        row_shape = jax.ShapeDtypeStruct((batch, rows, head_dim), jnp.bfloat16)
        shard_shape = jax.ShapeDtypeStruct((batch, shard_len, head_dim), jnp.bfloat16)
        dma, regular = pltpu.SemaphoreType.DMA, pltpu.SemaphoreType.REGULAR
        attn_out, grad_q, grad_k, grad_v, _ = pl.pallas_call(
            functools.partial(_kernel, ctx_size, heads),
            out_shape=[
                row_shape,
                row_shape,
                shard_shape,
                shard_shape,
                jax.ShapeDtypeStruct((batch, 2 * ctx_size, shard_len, head_dim), jnp.bfloat16),
            ],
            in_specs=[pl.BlockSpec(memory_space=pl.ANY)] * 4,
            out_specs=[pl.BlockSpec(memory_space=pl.ANY)] * 5,
            scratch_shapes=[
                pltpu.VMEM((2, 2, rows, head_dim), jnp.bfloat16),
                pltpu.VMEM((2, 2, rows, head_dim), jnp.bfloat16),
                pltpu.VMEM((2, 2, seq_len, head_dim), jnp.bfloat16),
                pltpu.VMEM((2, seq_len, head_dim), jnp.float32),
                pltpu.VMEM((2, ctx_size, shard_len, head_dim), jnp.float32),
                pltpu.VMEM((2, 2, 2, 4, shard_len, head_dim), jnp.float32),
                pltpu.VMEM((2, 2, shard_len, head_dim), jnp.bfloat16),
                dma((2, 2, 2, 4)),
                dma((2, 2, batch, 4)),
                dma((2, batch)),
                dma((batch,)),
                dma((batch,)),
                dma((2,)),
                dma((2,)),
                dma((2,)),
                dma((2, ctx_size // 2)),
                dma((2,)),
                dma((2, 2, 2, 4)),
                dma((2, 2)),
                dma((2,)),
                regular,
                regular((2,)),
            ]
            + _work_shapes(seq_len, head_dim, tile),
            compiler_params=pltpu.CompilerParams(vmem_limit_bytes=VMEM_BYTES, collective_id=0, has_side_effects=True),
            cost_estimate=pl.CostEstimate(flops=10**11, bytes_accessed=10**8, transcendentals=0),
        )(
            queries.reshape(batch, rows, head_dim),
            grad_out.reshape(batch, rows, head_dim),
            keys_in.reshape(batch, shard_len, head_dim),
            values_in.reshape(batch, shard_len, head_dim),
        )
        return attn_out.reshape(queries.shape), grad_q.reshape(queries.shape), grad_k.reshape(keys_in.shape), grad_v.reshape(values_in.shape)

    return jax.shard_map(local_attention, mesh=mesh, in_specs=(block_spec,) * 4, out_specs=(block_spec,) * 4, check_vma=False)
```
